32 devices in a mesh: seq: 8 (over z, y), mp: 4 (over x, core).
Axes of the slice: x: 2, y: 2, z: 4, core: 2. Of those that a mesh axis runs over, the one named last changes fastest.
Arguments:
- resid: bfloat16 [2048, 5120], P('seq', 'mp'), may hold values from -15 to 15
- queries: bfloat16 [2048, 5120], P('seq', 'mp'), may hold values from -28 to 28
- keys: bfloat16 [2048, 5120], P('seq', 'mp'), may hold values from -12.25 to 12.25
- values: bfloat16 [2048, 5120], P('seq', 'mp'), may hold values from -6 to 6
- doc_ids: int32 [2048], P('seq'), may hold values from 0 to 3, as said below
- out_proj: bfloat16 [5120, 5120], P('mp'), may hold values from -0.5 to 0.5
- ffn_gain: bfloat16 [5120], P('mp'), may hold values from 0.25 to 1.75
- w_in: bfloat16 [5120, 13824], P('mp', 'seq'), may hold values from -0.078125 to 0.078125
- w_out: bfloat16 [13824, 5120], P('seq', 'mp'), may hold values from -0.109375 to 0.109375
- hot_index: int32 [8, 384], P('seq'), may hold values from 0 to 1727, as said below
- hot_blocks: int32 [8], P('seq'), may hold values from 1 to 3, as said below
Outputs:
- layer_out: bfloat16 [2048, 5120], P('seq', 'mp')
- hot_mean: float32 [8, 384], P('seq')
The draws below stay inside these ranges and needn't reach their ends.
Inputs may be any that keep to these rules, and one draw needn't show every extreme that they name: `doc_ids`: document numbers never fall along the tokens; every number from 0 to 3 occurs; some document has 1024 tokens. `hot_index`: row g holds 384 distinct neuron numbers of group g; only its first 128 * hot_blocks[g] entries are live, the others are ignored. `hot_blocks`: some group has exactly 3 live blocks.
All inputs are finite; a program needn't handle non-finite values.
Results may differ from the reference program's by a relative error of at most 0.014.
Values may be sent and summed in bfloat16 or wider, within the bound.
A program may use at most 192 MiB of HBM per device.

```python
import jax
import jax.numpy as jnp
from jax import lax

D = 5120
HEADS = 40
HEAD_DIM = 128
FF = 13824
BLOCK = 128
CAP = 3
TOKENS = 2048
GROUPS = 8
NEURONS = 1728
SLOTS = 384


def paired_rows(key, which):
    noise = jnp.clip(jax.random.normal(jax.random.fold_in(key, 101 + which), (TOKENS, D), jnp.float32), -4.0, 4.0)
    return noise


def draw_resid(key, part):
    ramp = jnp.arange(D, dtype=jnp.float32) / (D - 1)
    rough = jnp.exp(jax.random.uniform(jax.random.fold_in(key, 501), (D,), jnp.float32, jnp.log(0.7), jnp.log(1.4)))
    column_scale = 0.5 * jnp.exp(ramp * jnp.log(5.0)) * rough
    noise = jnp.clip(jax.random.normal(jax.random.fold_in(key, 504), (TOKENS, D), jnp.float32), -4.0, 4.0)
    return (noise * column_scale[None, :]).astype(jnp.bfloat16)


def draw_queries(key, part):
    return paired_rows(key, 0).astype(jnp.bfloat16)


def draw_keys(key, part):
    return paired_rows(key, 1).astype(jnp.bfloat16)


def draw_doc_ids(key, part):
    half = TOKENS // 2
    cut_one = jax.random.randint(jax.random.fold_in(key, 401), (), 1, half - 1)
    cut_two = cut_one + half
    cut_three = jax.random.randint(jax.random.fold_in(key, 402), (), cut_two + 1, TOKENS)
    places = jnp.arange(TOKENS, dtype=jnp.int32)
    marks = (places >= cut_one).astype(jnp.int32) + (places >= cut_two).astype(jnp.int32) + (places >= cut_three).astype(jnp.int32)
    return marks.astype(jnp.int32)


def draw_hot_index(key, part):
    group_keys = jax.random.split(jax.random.fold_in(key, 201), GROUPS)
    orders = jax.vmap(lambda single: jax.random.permutation(single, NEURONS))(group_keys)
    return orders[:, :SLOTS].astype(jnp.int32)


def draw_hot_blocks(key, part):
    busy = jax.random.randint(jax.random.fold_in(key, 301), (GROUPS,), 0, 3) == 0
    extra = jax.random.randint(jax.random.fold_in(key, 302), (GROUPS,), 2, CAP + 1)
    counts = jnp.where(busy, extra, 1)
    heaviest = jax.random.randint(jax.random.fold_in(key, 303), (), 0, GROUPS)
    return jnp.where(jnp.arange(GROUPS) == heaviest, CAP, counts).astype(jnp.int32)


def block_levels(stream_key, shape, cuts, least, largest):
    level = 1.0
    for position, parts in cuts:
        steps = jax.random.uniform(jax.random.fold_in(jax.random.fold_in(stream_key, 6), position), (parts,), jnp.float32, least / len(cuts), largest / len(cuts))
        level = level * jnp.repeat(jnp.exp(steps), shape[position] // parts).reshape((-1,) + (1,) * (len(shape) - 1 - position))
    return level


def bell_draw(stream_key, shape, deviation, bound, shards=(), kind=jnp.bfloat16):
    factor_of = block_levels(stream_key, shape, shards, -0.22, 0.18) if shards else 1.0
    values = jax.random.normal(stream_key, shape, jnp.float32) * deviation * factor_of
    return jnp.minimum(jnp.maximum(values, -bound), bound).astype(kind)


def setup_inputs(seed: int = 0) -> dict:
    splits = jax.random.split(jax.random.key(seed), 12)
    return {
        "resid": draw_resid(jax.random.fold_in(splits[11], 71), 0),
        "queries": draw_queries(jax.random.fold_in(splits[11], 71), 0),
        "keys": draw_keys(jax.random.fold_in(splits[11], 71), 0),
        "values": bell_draw(splits[3], (TOKENS, D), 1.0, 6.0, ((0, 8), (1, 4))),
        "doc_ids": draw_doc_ids(jax.random.fold_in(splits[11], 71), 0),
        "out_proj": bell_draw(splits[5], (D, D), HEAD_DIM ** -0.5, 0.5, ((0, 4),)),
        "ffn_gain": jnp.clip(1.0 + 0.15 * jax.random.normal(splits[6], (D,), jnp.float32), 0.25, 1.75).astype(jnp.bfloat16),
        "w_in": bell_draw(splits[7], (D, FF), D ** -0.5, 0.078125, ((0, 4), (1, 8))),
        "w_out": bell_draw(splits[8], (FF, D), (FF // 4) ** -0.5, 0.109375, ((0, 8), (1, 4))),
        "hot_index": draw_hot_index(jax.random.fold_in(splits[11], 71), 0),
        "hot_blocks": draw_hot_blocks(jax.random.fold_in(splits[11], 71), 0),
    }


epsilon = 1e-05
masked_score = -1e+30

def reference(resid, queries, keys, values, doc_ids, out_proj, ffn_gain, w_in, w_out, hot_index, hot_blocks):
    scale = HEAD_DIM ** (-0.5)
    positions = jnp.arange(TOKENS, dtype=jnp.int32)
    visible = (positions[:, None] >= positions[None, :]) & (doc_ids[:, None] == doc_ids[None, :])

    def one_head(triple):
        query_head, key_head, value_head = triple
        scores = jnp.dot(query_head, key_head.T, preferred_element_type=jnp.float32) * scale
        scores = jnp.where(visible, scores, masked_score)
        top = lax.optimization_barrier(jnp.max(scores, axis=1, keepdims=True))
        weights = jnp.where(visible, jnp.exp(scores - top), 0.0)
        total = lax.optimization_barrier(jnp.sum(weights, axis=1, keepdims=True))
        mixed = jnp.dot(weights.astype(jnp.bfloat16), value_head, preferred_element_type=jnp.float32)
        return (mixed / total).astype(jnp.bfloat16)
    split_queries = queries.reshape(TOKENS, HEADS, HEAD_DIM).transpose(1, 0, 2)
    split_keys = keys.reshape(TOKENS, HEADS, HEAD_DIM).transpose(1, 0, 2)
    split_values = values.reshape(TOKENS, HEADS, HEAD_DIM).transpose(1, 0, 2)
    attended = lax.map(one_head, (split_queries, split_keys, split_values))
    attended = attended.transpose(1, 0, 2).reshape(TOKENS, D)
    projected = jnp.dot(attended, out_proj, preferred_element_type=jnp.float32)
    state_rows = (resid.astype(jnp.float32) + projected).astype(jnp.bfloat16)
    widened = state_rows.astype(jnp.float32)
    inverse = lax.rsqrt(lax.optimization_barrier(jnp.mean(widened * widened, axis=1, keepdims=True)) + epsilon)
    normed = (widened * inverse * ffn_gain.astype(jnp.float32)).astype(jnp.bfloat16)
    slot_ids = jnp.arange(SLOTS, dtype=jnp.int32)

    def one_group(carry, group):
        columns = (group * NEURONS + hot_index[group]).astype(jnp.int32)
        live = slot_ids < BLOCK * hot_blocks[group]
        before = jnp.dot(normed, jnp.take(w_in, columns, axis=1), preferred_element_type=jnp.float32)
        active = jnp.where(live[None, :], jnp.maximum(before, 0.0), 0.0)
        carry = carry + jnp.dot(active.astype(jnp.bfloat16), jnp.take(w_out, columns, axis=0), preferred_element_type=jnp.float32)
        return (carry, lax.optimization_barrier(jnp.mean(active, axis=0)))
    ffn_sum, hot_mean = lax.scan(one_group, jnp.zeros((TOKENS, D), jnp.float32), jnp.arange(GROUPS, dtype=jnp.int32))
    layer_out = (widened + ffn_sum).astype(jnp.bfloat16)
    return (layer_out, hot_mean)
```

```python
import functools

import jax
import jax.numpy as jnp
from jax import lax
from jax.experimental import pallas as pl
from jax.experimental.pallas import tpu as pltpu
from jax.sharding import PartitionSpec as P

HEAD_DIM = 128
BLOCK = 128
MESH = pl.DeviceIdType.MESH
VMEM = pltpu.VMEM

epsilon = 1e-05
masked_score = -1e30


def row_length(mesh):
    seq = mesh.shape["seq"]
    try:
        first = [mesh.devices[i, 0].coords for i in range(seq)]
        size = len({c[1] for c in first})
        if seq % size == 0:
            return size
    except (AttributeError, IndexError, TypeError):
        pass
    return 2


def gather_kernel(nz, ny, up, down, window, chunks, count, *refs):
    ins = refs[:count]
    outs = refs[count : 2 * count]
    sems = refs[2 * count :]
    own_sem, zs_sem, zr_sem, ys_sem, yr_sem = sems
    me = lax.axis_index("seq")
    mp = lax.axis_index("mp")
    z = me // ny
    y = me % ny

    def dev(zz, yy):
        return (zz * ny + yy, mp)

    barrier = pltpu.get_barrier_semaphore()
    for step in (-1, 1):
        ok = (z + step >= 0) & (z + step < nz)

        @pl.when(ok)
        def _(step=step):
            pl.semaphore_signal(barrier, inc=1, device_id=dev(z + step, y), device_id_type=MESH)

    for dy in range(1, ny):
        pl.semaphore_signal(
            barrier, inc=1, device_id=dev(z, (y + dy) % ny), device_id_type=MESH
        )
    below = jnp.where(z > 0, 1, 0)
    above = jnp.where(z < nz - 1, 1, 0)
    pl.semaphore_wait(barrier, below + above + ny - 1)

    def piece(ref, a, c):
        rows = ins[a].shape[0]
        if chunks[a] == 1:
            return ref
        size = rows // chunks[a]
        return ref.at[pl.ds(c * size, size)]

    def slot(a, zz, yy, c):
        return piece(outs[a].at[zz * ny + yy], a, c)

    base = []
    total = 0
    for a in range(count):
        base.append(total)
        total += chunks[a]

    def own_copy(a):
        return pltpu.make_async_copy(ins[a], outs[a].at[me], own_sem.at[a])

    def level_z(lv):
        return z - lv if lv <= up else z + (lv - up)

    def source(lv, a, c):
        if lv == 0:
            return piece(ins[a], a, c)
        return slot(a, level_z(lv), y, c)

    def z_copy(lv, direction, a, c):
        there = (lv + 1) if direction > 0 else (up + 1 if lv == 0 else lv + 1)
        return pltpu.make_async_remote_copy(
            src_ref=source(lv, a, c),
            dst_ref=slot(a, level_z(lv), y, c),
            send_sem=zs_sem.at[there - 1, base[a] + c],
            recv_sem=zr_sem.at[there - 1, base[a] + c],
            device_id=dev(z + direction, y),
            device_id_type=MESH,
        )

    def z_cond(lv, direction):
        src = level_z(lv)
        return (src >= 0) & (src < nz) & (z + direction >= 0) & (z + direction < nz)

    def y_needed(lv, y_from, y_to):
        src = level_z(lv)
        ok = (src >= 0) & (src < nz)
        if window is not None:
            offset = (z - src) * ny + y_to - y_from
            ok = ok & (offset >= 0) & (offset <= window)
        return ok

    def y_copy(lv, dy, a, c):
        return pltpu.make_async_remote_copy(
            src_ref=source(lv, a, c),
            dst_ref=slot(a, level_z(lv), y, c),
            send_sem=ys_sem.at[lv * (ny - 1) + dy - 1, base[a] + c],
            recv_sem=yr_sem.at[lv * (ny - 1) + dy - 1, base[a] + c],
            device_id=dev(z, (y + dy) % ny),
            device_id_type=MESH,
        )

    def y_arrival(lv, dy, a, c):
        return pltpu.make_async_remote_copy(
            src_ref=source(lv, a, c),
            dst_ref=slot(a, level_z(lv), (y + ny - dy) % ny, c),
            send_sem=ys_sem.at[lv * (ny - 1) + dy - 1, base[a] + c],
            recv_sem=yr_sem.at[lv * (ny - 1) + dy - 1, base[a] + c],
            device_id=dev(z, (y + dy) % ny),
            device_id_type=MESH,
        )

    every = [(a, c) for a in range(count) for c in range(chunks[a])]

    def directions(lv):
        out = []
        if lv < up:
            out.append(1)
        if down and (lv == 0 or (lv > up and lv - up < down)):
            out.append(-1)
        return out

    def spread(lv, a, c):
        for direction in directions(lv):

            @pl.when(z_cond(lv, direction))
            def _(direction=direction):
                z_copy(lv, direction, a, c).start()

        for dy in range(1, ny):

            @pl.when(y_needed(lv, y, (y + dy) % ny))
            def _(dy=dy):
                y_copy(lv, dy, a, c).start()

    for a, c in every:
        spread(0, a, c)
    for a in range(count):
        own_copy(a).start()
    order = []
    for k in range(1, max(up, down) + 1):
        for a, c in every:
            if k <= up:
                order.append((k, a, c))
            if k <= down:
                order.append((up + k, a, c))
    for lv, a, c in order:
        src = level_z(lv)

        @pl.when((src >= 0) & (src < nz))
        def _(lv=lv, a=a, c=c):
            pltpu.make_async_remote_copy(
                src_ref=slot(a, level_z(lv), y, c),
                dst_ref=slot(a, level_z(lv), y, c),
                send_sem=zs_sem.at[lv - 1, base[a] + c],
                recv_sem=zr_sem.at[lv - 1, base[a] + c],
                device_id=dev(z, (y + 1) % ny),
                device_id_type=MESH,
            ).wait_recv()
            spread(lv, a, c)

    for lv in range(up + down + 1):
        for a, c in every:
            for dy in range(1, ny):

                @pl.when(y_needed(lv, (y + ny - dy) % ny, y))
                def _(lv=lv, a=a, c=c, dy=dy):
                    y_arrival(lv, dy, a, c).wait_recv()

    for lv in range(up + down + 1):
        for a, c in every:
            for direction in directions(lv):

                @pl.when(z_cond(lv, direction))
                def _(lv=lv, a=a, c=c, direction=direction):
                    z_copy(lv, direction, a, c).wait_send()

            for dy in range(1, ny):

                @pl.when(y_needed(lv, y, (y + dy) % ny))
                def _(lv=lv, a=a, c=c, dy=dy):
                    y_copy(lv, dy, a, c).wait_send()

    for a in range(count):
        own_copy(a).wait()


def seq_gather(arrays, ny, causal, chunks, collective_id):
    n = lax.axis_size("seq")
    nz = n // ny
    if causal:
        window = n // 2
        up, down = min(nz - 1, -(-window // ny)), 0
    else:
        window = None
        up = down = nz - 1
    count = len(arrays)
    total = sum(chunks)
    levels = up + down
    return pl.pallas_call(
        functools.partial(gather_kernel, nz, ny, up, down, window, chunks, count),
        out_shape=[jax.ShapeDtypeStruct((n,) + a.shape, a.dtype) for a in arrays],
        in_specs=[pl.BlockSpec(memory_space=VMEM)] * count,
        out_specs=[pl.BlockSpec(memory_space=pl.ANY)] * count,
        scratch_shapes=[
            pltpu.SemaphoreType.DMA((count,)),
            pltpu.SemaphoreType.DMA((levels, total)),
            pltpu.SemaphoreType.DMA((levels, total)),
            pltpu.SemaphoreType.DMA(((levels + 1) * (ny - 1), total)),
            pltpu.SemaphoreType.DMA(((levels + 1) * (ny - 1), total)),
        ],
        compiler_params=pltpu.CompilerParams(
            collective_id=collective_id, has_side_effects=True
        ),
    )(*arrays)


def attention_kernel(window, scale, q_ref, k_ref, v_ref, qdoc_ref, kdoc_ref, out_ref):
    here = lax.axis_index("seq")
    rows = q_ref.shape[0]
    query = q_ref[...]
    query_doc = qdoc_ref[...]
    row = lax.broadcasted_iota(jnp.int32, (rows, rows), 0)
    col = lax.broadcasted_iota(jnp.int32, (rows, rows), 1)
    first = jnp.maximum(here - window, 0)

    def visit(block, carry):
        top, total, accum = carry
        scores = (
            lax.dot_general(
                query,
                k_ref[block],
                (((1,), (1,)), ((), ())),
                preferred_element_type=jnp.float32,
            )
            * scale
        )
        visible = (query_doc == kdoc_ref[block, 0:1, :]) & (
            row - col >= (block - here) * rows
        )
        scores = jnp.where(visible, scores, masked_score)
        new_top = jnp.maximum(top, jnp.max(scores, axis=1, keepdims=True))
        weights = jnp.where(visible, jnp.exp(scores - new_top), 0.0)
        fade = jnp.exp(top - new_top)
        total = total * fade + jnp.sum(weights, axis=1, keepdims=True)
        accum = accum * fade + jnp.dot(
            weights.astype(jnp.bfloat16), v_ref[block], preferred_element_type=jnp.float32
        )
        return new_top, total, accum

    start = (
        jnp.full((rows, 1), masked_score, jnp.float32),
        jnp.zeros((rows, 1), jnp.float32),
        jnp.zeros((rows, HEAD_DIM), jnp.float32),
    )
    _, total, accum = lax.fori_loop(first, here + 1, visit, start)
    out_ref[...] = (accum / total).astype(jnp.bfloat16)


def attention(queries, keys, values, doc_col, doc_rows):
    rows, width = queries.shape
    n = keys.shape[0]
    heads = width // HEAD_DIM
    return pl.pallas_call(
        functools.partial(attention_kernel, n // 2, HEAD_DIM ** (-0.5)),
        grid=(heads,),
        out_shape=jax.ShapeDtypeStruct((rows, width), jnp.bfloat16),
        in_specs=[
            pl.BlockSpec((rows, HEAD_DIM), lambda h: (0, h)),
            pl.BlockSpec((n, rows, HEAD_DIM), lambda h: (0, 0, h)),
            pl.BlockSpec((n, rows, HEAD_DIM), lambda h: (0, 0, h)),
            pl.BlockSpec((rows, 1), lambda h: (0, 0)),
            pl.BlockSpec(doc_rows.shape, lambda h: (0, 0, 0)),
        ],
        out_specs=pl.BlockSpec((rows, HEAD_DIM), lambda h: (0, h)),
    )(queries, keys, values, doc_col, doc_rows)


def mp_scatter_kernel(n, ny, x_ref, w_ref, out_ref, all_ref, near, sums, far, s1, r1, s2, r2, ws, wr, own_sem):
    seq = lax.axis_index("seq")
    me = lax.axis_index("mp")
    z = seq // ny
    y = seq % ny
    chips = n // 2
    chip = me // 2
    core = me % 2
    partner = chip * 2 + 1 - core
    width = out_ref.shape[1]
    slots = w_ref.shape[1]
    barrier = pltpu.get_barrier_semaphore()
    pl.semaphore_signal(barrier, inc=1, device_id=(seq, partner), device_id_type=MESH)
    for d in range(1, chips):
        other = ((chip + d) % chips) * 2 + core
        pl.semaphore_signal(barrier, inc=1, device_id=(seq, other), device_id_type=MESH)
    for d in range(1, ny):
        pl.semaphore_signal(
            barrier, inc=1, device_id=(z * ny + (y + d) % ny, me), device_id_type=MESH
        )
    pl.semaphore_wait(barrier, chips + ny - 1)

    def columns(index):
        return pl.ds(pl.multiple_of(index * width, 128), width)

    first = []
    for d in list(range(1, chips)) + [0]:
        target = (chip + d) % chips
        copy = pltpu.make_async_remote_copy(
            src_ref=x_ref.at[:, columns(target * 2 + 1 - core)],
            dst_ref=near.at[d],
            send_sem=s1.at[d],
            recv_sem=r1.at[d],
            device_id=(seq, partner),
            device_id_type=MESH,
        )
        copy.start()
        first.append((d, target, copy))
    shared = []
    for d in range(1, ny):
        copy = pltpu.make_async_remote_copy(
            src_ref=w_ref,
            dst_ref=all_ref.at[:, pl.ds(d * slots, slots)],
            send_sem=ws.at[d - 1],
            recv_sem=wr.at[d - 1],
            device_id=(z * ny + (y + ny - d) % ny, me),
            device_id_type=MESH,
        )
        copy.start()
        shared.append(copy)
    own = pltpu.make_async_copy(w_ref, all_ref.at[:, pl.ds(0, slots)], own_sem)
    own.start()
    second = []
    for d, target, copy in first:
        copy.wait_recv()
        mine = x_ref[:, columns(target * 2 + core)].astype(jnp.float32)
        total = mine + near[d].astype(jnp.float32)
        if d == 0:
            out_ref[...] = total
            continue
        sums[d - 1] = total.astype(jnp.bfloat16)
        send = pltpu.make_async_remote_copy(
            src_ref=sums.at[d - 1],
            dst_ref=far.at[d - 1],
            send_sem=s2.at[d - 1],
            recv_sem=r2.at[d - 1],
            device_id=(seq, target * 2 + core),
            device_id_type=MESH,
        )
        send.start()
        second.append((d, send))
    for d, send in second:
        send.wait_recv()
        out_ref[...] += far[d - 1].astype(jnp.float32)
    for copy in shared:
        copy.wait_recv()
    for d, target, copy in first:
        copy.wait_send()
    for d, send in second:
        send.wait_send()
    for copy in shared:
        copy.wait_send()
    own.wait()


def mp_scatter(x, hot_in, ny, collective_id):
    n = lax.axis_size("mp")
    rows, total = x.shape
    width = total // n
    chips = n // 2
    depth, slots = hot_in.shape
    dma = pltpu.SemaphoreType.DMA
    return pl.pallas_call(
        functools.partial(mp_scatter_kernel, n, ny),
        out_shape=[
            jax.ShapeDtypeStruct((rows, width), jnp.float32),
            jax.ShapeDtypeStruct((depth, ny * slots), jnp.bfloat16),
        ],
        in_specs=[pl.BlockSpec(memory_space=VMEM)] * 2,
        out_specs=[pl.BlockSpec(memory_space=VMEM), pl.BlockSpec(memory_space=pl.ANY)],
        scratch_shapes=[
            VMEM((chips, rows, width), jnp.bfloat16),
            VMEM((chips - 1, rows, width), jnp.bfloat16),
            VMEM((chips - 1, rows, width), jnp.bfloat16),
            dma((chips,)),
            dma((chips,)),
            dma((chips - 1,)),
            dma((chips - 1,)),
            dma((ny - 1,)),
            dma((ny - 1,)),
            dma,
        ],
        compiler_params=pltpu.CompilerParams(
            collective_id=collective_id, has_side_effects=True, vmem_limit_bytes=48 * 1024 * 1024
        ),
    )(x, hot_in)


def ffn_kernel(
    nz, ny, nmp, count, total_tokens,
    x_ref, state_ref, win_ref, wout_ref, out_ref, mean_ref,
    win, wout, gathered, part, own_part, near, pair, active, contrib, moving, from_below, from_above,
    hot, hot_near, hot_send, hot_other,
    load_sem, ag_s, ag_r, pd_s, pd_r, px_s, px_r, ad_s, ad_r, up_s, up_r, dn_s, dn_r, wo_s, wo_r, hp_s, hp_r, hy_s, hy_r,
):
    f32 = jnp.float32
    bf16 = jnp.bfloat16
    seq = lax.axis_index("seq")
    me = lax.axis_index("mp")
    z = seq // ny
    y = seq % ny
    chips = nmp // 2
    chip = me // 2
    core = me % 2
    rows, width = x_ref.shape
    slots = wout_ref.shape[0]
    size = rows // count
    half = nz // 2
    span = half * size
    last = nz - 1
    partner = (seq, chip * 2 + 1 - core)

    def at_z(step):
        return ((z + step) * ny + y, me)

    def at_y(d):
        return (z * ny + (y + d) % ny, me)

    def at_x(d):
        return (seq, ((chip + d) % chips) * 2 + core)

    barrier = pltpu.get_barrier_semaphore()

    def greet(where):
        pl.semaphore_signal(barrier, inc=1, device_id=where, device_id_type=MESH)

    @pl.when(z > 0)
    def _():
        greet(at_z(-1))

    @pl.when(z < last)
    def _():
        greet(at_z(1))

    greet(partner)
    for d in range(1, chips):
        greet(at_x(d))
    for d in range(1, ny):
        greet(at_y(d))
    below = jnp.where(z > 0, 1, 0)
    above = jnp.where(z < last, 1, 0)
    pl.semaphore_wait(barrier, below + above + chips + ny - 1)

    def remote(src, dst, send, recv, where):
        return pltpu.make_async_remote_copy(
            src_ref=src, dst_ref=dst, send_sem=send, recv_sem=recv,
            device_id=where, device_id_type=MESH,
        )

    def own_rows(c):
        return x_ref.at[pl.ds(c * size, size)]

    def gather_copy(step, k, c):
        block = z - step * k
        src = own_rows(c) if k == 0 else gathered.at[c, block]
        way = 0 if step > 0 else 1
        return remote(src, gathered.at[c, block], ag_s.at[way, k, c], ag_r.at[block, c], at_z(step))

    def can_pass(step, k):
        block = z - step * k
        there = z + step
        return (block >= 0) & (block < nz) & (there >= 0) & (there < nz)

    def pass_on(k, c, steps=(1, -1)):
        for step in steps:

            @pl.when(can_pass(step, k))
            def _(step=step):
                gather_copy(step, k, c).start()

    def own_send(c):
        pass_on(0, c)

    def collect(c):
        gathered[c, z] = x_ref[pl.ds(c * size, size), :]
        for k in range(1, nz):
            for step in (1, -1):
                block = z - step * k

                @pl.when((block >= 0) & (block < nz))
                def _(step=step, k=k, block=block):
                    remote(
                        gathered.at[c, block], gathered.at[c, block],
                        ag_s.at[0, 0, c], ag_r.at[block, c], partner,
                    ).wait_recv()
                    if k < nz - 1:
                        pass_on(k, c, (step,))

    def half_rows(side):
        return pl.ds(side * half, half)

    def pre_copy(c):
        return remote(part.at[c], near.at[c], pd_s.at[c], pd_r.at[c], partner)

    def multiply_in(c):
        other = gathered[c, half_rows(1 - core)].reshape(span, width)
        part[c] = jnp.dot(other, win[...], preferred_element_type=f32).astype(bf16)
        pre_copy(c).start()
        mine = gathered[c, half_rows(core)].reshape(span, width)
        own_part[c] = jnp.dot(mine, win[...], preferred_element_type=f32)

    def across_copy(d, c):
        return remote(
            pair.at[c, chip], pair.at[c, chip], px_s.at[d - 1, c], px_r.at[chip, c], at_x(d)
        )

    def exchange(c):
        pre_copy(c).wait_recv()
        pair[c, chip] = (own_part[c] + near[c].astype(f32)).astype(bf16)
        for d in range(1, chips):
            across_copy(d, c).start()

    def active_copy(c):
        return remote(
            active.at[c, half_rows(core)], active.at[c, half_rows(core)],
            ad_s.at[c], ad_r.at[c], partner,
        )

    def activate(c):
        for d in range(1, chips):
            other = (chip + d) % chips
            remote(
                pair.at[c, other], pair.at[c, other], px_s.at[d - 1, c], px_r.at[other, c], at_x(d)
            ).wait_recv()
        pre = pair[c, 0].astype(f32)
        for k in range(1, chips):
            pre = pre + pair[c, k].astype(f32)
        value = jnp.maximum(pre, 0.0)
        active[c, half_rows(core)] = value.astype(bf16).reshape(half, size, value.shape[1])
        active_copy(c).start()
        hot[...] += jnp.sum(value.reshape(span // 8, 8, value.shape[1]), axis=0)

    def up_copy(t, c):
        return remote(moving.at[c, t], from_below.at[c, t], up_s.at[t, c], up_r.at[t, c], at_z(1))

    def down_copy(t, c):
        return remote(moving.at[c, t], from_above.at[c, t], dn_s.at[t, c], dn_r.at[t, c], at_z(-1))

    def multiply_out(c):
        other = half_rows(1 - core)
        remote(active.at[c, other], active.at[c, other], ad_s.at[c], ad_r.at[c], partner).wait_recv()
        lhs = active[c].reshape(nz * size, active.shape[3])
        contrib[c] = jnp.dot(lhs, wout[...], preferred_element_type=f32).reshape(nz, size, width)

        @pl.when(z == 0)
        def _():
            for t in range(last, 0, -1):
                moving[c, t] = contrib[c, t].astype(bf16)
                up_copy(t, c).start()

        @pl.when(z == last)
        def _():
            for t in range(last):
                moving[c, t] = contrib[c, t].astype(bf16)
                down_copy(t, c).start()

    def middle(c):
        for k in range(nz - 1, 0, -1):
            up = z + k

            @pl.when((z > 0) & (up < nz))
            def _(up=up):
                up_copy(up, c).wait_recv()
                moving[c, up] = (contrib[c, up] + from_below[c, up].astype(f32)).astype(bf16)
                up_copy(up, c).start()

            down = z - k

            @pl.when((z < last) & (down >= 0))
            def _(down=down):
                down_copy(down, c).wait_recv()
                moving[c, down] = (contrib[c, down] + from_above[c, down].astype(f32)).astype(bf16)
                down_copy(down, c).start()

    def finish(c):
        @pl.when(z > 0)
        def _():
            up_copy(z, c).wait_recv()
            contrib[c, z] += from_below[c, z].astype(f32)

        @pl.when(z < last)
        def _():
            down_copy(z, c).wait_recv()
            contrib[c, z] += from_above[c, z].astype(f32)

        here = pl.ds(c * size, size)
        out_ref[here, :] = (state_ref[here, :].astype(f32) + contrib[c, z]).astype(bf16)

    def wout_copy(d):
        return remote(
            wout_ref, wout.at[pl.ds(d * slots, slots)], wo_s.at[d - 1], wo_r.at[d - 1], at_y(ny - d)
        )

    own_send(0)
    load_in = pltpu.make_async_copy(win_ref, win, load_sem.at[0])
    load_in.start()
    load_out = pltpu.make_async_copy(wout_ref, wout.at[pl.ds(0, slots)], load_sem.at[1])
    load_out.start()
    for d in range(1, ny):
        wout_copy(d).start()
    own_send(1)
    hot[...] = jnp.zeros_like(hot)
    for i in range(count + 2):
        if i < count:
            collect(i)
            if i + 2 < count:
                own_send(i + 2)
            if i == 0:
                load_in.wait()
            multiply_in(i)
        if 1 <= i <= count:
            activate(i - 1)
        if i < count:
            exchange(i)
        if i == 1:
            load_out.wait()
            for d in range(1, ny):
                wout_copy(d).wait_recv()
        if 1 <= i <= count:
            multiply_out(i - 1)
        if i >= 2:
            middle(i - 2)

    hot_pair = remote(hot, hot_near, hp_s, hp_r, partner)
    hot_pair.start()
    hot_pair.wait_recv()
    both = jnp.sum(hot[...] + hot_near[...], axis=0, keepdims=True)
    hot_send[...] = jnp.broadcast_to(both, hot_send.shape)

    def mean_copy(d):
        return remote(
            hot_send.at[:, pl.ds(d * slots, slots)], hot_other.at[d - 1],
            hy_s.at[d - 1], hy_r.at[d - 1], at_y(d),
        )

    for d in range(1, ny):
        mean_copy(d).start()
    for c in range(count):
        finish(c)
    total = hot_send[0:1, 0:slots]
    for d in range(1, ny):
        mean_copy(d).wait_recv()
        total = total + hot_other[d - 1, 0:1, :]
    mean_ref[...] = total / total_tokens

    for c in range(count):
        for k in range(nz - 1):
            for step in (1, -1):

                @pl.when(can_pass(step, k))
                def _(step=step, k=k, c=c):
                    gather_copy(step, k, c).wait_send()

        pre_copy(c).wait_send()
        for d in range(1, chips):
            across_copy(d, c).wait_send()
        active_copy(c).wait_send()
        for t in range(nz):

            @pl.when((t > z) & (z < last))
            def _(t=t, c=c):
                up_copy(t, c).wait_send()

            @pl.when((t < z) & (z > 0))
            def _(t=t, c=c):
                down_copy(t, c).wait_send()

    for d in range(1, ny):
        wout_copy(d).wait_send()
        mean_copy(d).wait_send()
    hot_pair.wait_send()


def ffn(normed, state, win, wout, ny, count, total_tokens, collective_id):
    rows, width = normed.shape
    slots = wout.shape[0]
    n = lax.axis_size("seq")
    nmp = lax.axis_size("mp")
    nz = n // ny
    chips = nmp // 2
    size = rows // count
    span = (nz // 2) * size
    wide = ny * slots
    dma = pltpu.SemaphoreType.DMA
    vmem = pl.BlockSpec(memory_space=VMEM)
    anywhere = pl.BlockSpec(memory_space=pl.ANY)
    f32 = jnp.float32
    bf16 = jnp.bfloat16
    return pl.pallas_call(
        functools.partial(ffn_kernel, nz, ny, nmp, count, total_tokens),
        out_shape=[
            jax.ShapeDtypeStruct((rows, width), bf16),
            jax.ShapeDtypeStruct((1, slots), f32),
        ],
        in_specs=[vmem, vmem, anywhere, anywhere],
        out_specs=[vmem, vmem],
        scratch_shapes=[
            VMEM((width, wide), bf16),
            VMEM((wide, width), bf16),
            VMEM((count, nz, size, width), bf16),
            VMEM((count, span, wide), bf16),
            VMEM((count, span, wide), f32),
            VMEM((count, span, wide), bf16),
            VMEM((count, chips, span, wide), bf16),
            VMEM((count, nz, size, wide), bf16),
            VMEM((count, nz, size, width), f32),
            VMEM((count, nz, size, width), bf16),
            VMEM((count, nz, size, width), bf16),
            VMEM((count, nz, size, width), bf16),
            VMEM((8, wide), f32),
            VMEM((8, wide), f32),
            VMEM((8, wide), f32),
            VMEM((ny - 1, 8, slots), f32),
            dma((2,)),
            dma((2, nz, count)),
            dma((nz, count)),
            dma((count,)),
            dma((count,)),
            dma((chips - 1, count)),
            dma((chips, count)),
            dma((count,)),
            dma((count,)),
            dma((nz, count)),
            dma((nz, count)),
            dma((nz, count)),
            dma((nz, count)),
            dma((ny - 1,)),
            dma((ny - 1,)),
            dma,
            dma,
            dma((ny - 1,)),
            dma((ny - 1,)),
        ],
        compiler_params=pltpu.CompilerParams(
            collective_id=collective_id, has_side_effects=True, vmem_limit_bytes=60 * 1024 * 1024
        ),
    )(normed, state, win, wout)


def local(
    ny,
    resid,
    queries,
    keys,
    values,
    doc_ids,
    out_proj,
    ffn_gain,
    w_in,
    w_out,
    hot_index,
    hot_blocks,
):
    tok_dev, width_dev = resid.shape
    groups = lax.axis_size("seq")
    width = width_dev * lax.axis_size("mp")
    total_tokens = tok_dev * groups
    doc_row = jnp.broadcast_to(doc_ids[None, :], (8, tok_dev))
    doc_rows, all_keys, all_values = seq_gather(
        [doc_row, keys, values], ny, True, (1, 2, 2), 0
    )
    chosen = hot_index[0]
    slots = chosen.shape[0]
    live = jnp.arange(slots, dtype=jnp.int32) < BLOCK * hot_blocks[0]
    neurons = jnp.arange(w_in.shape[1], dtype=jnp.int32)
    picks = ((neurons[:, None] == chosen[None, :]) & live[None, :]).astype(jnp.bfloat16)
    hot_in = jnp.dot(w_in, picks, preferred_element_type=jnp.float32).astype(jnp.bfloat16)
    hot_out = lax.dot_general(
        picks, w_out, (((0,), (0,)), ((), ())), preferred_element_type=jnp.float32
    ).astype(jnp.bfloat16)
    attended = attention(queries, all_keys, all_values, doc_ids[:, None], doc_rows)
    projected = jnp.dot(attended, out_proj, preferred_element_type=jnp.float32)
    projected, win = mp_scatter(projected.astype(jnp.bfloat16), hot_in, ny, 1)
    state_rows = (resid.astype(jnp.float32) + projected).astype(jnp.bfloat16)
    widened = state_rows.astype(jnp.float32)
    squares = lax.psum(jnp.sum(widened * widened, axis=1), "mp")
    inverse = lax.rsqrt(squares / width + epsilon)
    normed = (widened * inverse[:, None] * ffn_gain.astype(jnp.float32)).astype(jnp.bfloat16)
    return ffn(normed, state_rows, win, hot_out, ny, 4, total_tokens, 2)


def solution(mesh):
    return jax.shard_map(
        functools.partial(local, row_length(mesh)),
        mesh=mesh,
        in_specs=(
            P("seq", "mp"),
            P("seq", "mp"),
            P("seq", "mp"),
            P("seq", "mp"),
            P("seq"),
            P("mp", None),
            P("mp"),
            P("mp", "seq"),
            P("seq", "mp"),
            P("seq", None),
            P("seq"),
        ),
        out_specs=(P("seq", "mp"), P("seq", None)),
        check_vma=False,
    )
```

```python
import functools

import jax
import jax.numpy as jnp
from jax import lax
from jax.experimental import pallas as pl
from jax.experimental.pallas import tpu as pltpu
from jax.sharding import PartitionSpec as P

HEAD_DIM = 128
BLOCK = 128
MESH = pl.DeviceIdType.MESH
VMEM = pltpu.VMEM

epsilon = 1e-05
masked_score = -1e30


def row_length(mesh):
    seq = mesh.shape["seq"]
    try:
        first = [mesh.devices[i, 0].coords for i in range(seq)]
        size = len({c[1] for c in first})
        if seq % size == 0:
            return size
    except (AttributeError, IndexError, TypeError):
        pass
    return 2


def front_kernel(
    nz, ny, nmp, up, window, per, scale,
    q_ref, k_ref, v_ref, doc_ref, qdoc_ref, resid_ref, gain_ref, row_ref, col_ref, win_hbm, wout_hbm, proj_hbm,
    state_ref, normed_ref, all_ref, hot_out_ref,
    kbuf, vbuf, docs, bias, scores, attended, proj, win, wout, hot_in,
    far_part, near_part, far_near, near_near, sums, far, total, squares,
    load_sem, z_s, y_s, recv, f_s, f_r, n_s, n_r, x_s, x_r, q_s, q_r, w_s, w_r, own_sem,
):
    f32 = jnp.float32
    bf16 = jnp.bfloat16
    seq = lax.axis_index("seq")
    me = lax.axis_index("mp")
    z = seq // ny
    y = seq % ny
    chips = nmp // 2
    chip = me // 2
    core = me % 2
    rows, width = q_ref.shape
    wide = per * HEAD_DIM
    count = width // wide
    slots = row_ref.shape[1]
    last = nz - 1
    partner = (seq, chip * 2 + 1 - core)

    barrier = pltpu.get_barrier_semaphore()

    def greet(where):
        pl.semaphore_signal(barrier, inc=1, device_id=where, device_id_type=MESH)

    above = ((z + 1) * ny + y, me)

    @pl.when(z > 0)
    def _():
        greet(((z - 1) * ny + y, me))

    @pl.when(z < last)
    def _():
        greet(above)

    for d in range(1, nmp):
        greet((seq, (me + d) % nmp))
    for d in range(1, ny):
        greet((z * ny + (y + d) % ny, me))
    has_below = jnp.where(z > 0, 1, 0)
    has_above = jnp.where(z < last, 1, 0)
    pl.semaphore_wait(barrier, has_below + has_above + nmp + ny - 2)

    def remote(src, dst, send, got, where):
        return pltpu.make_async_remote_copy(
            src_ref=src, dst_ref=dst, send_sem=send, recv_sem=got,
            device_id=where, device_id_type=MESH,
        )

    def cols(c):
        return pl.ds(pl.multiple_of(c * wide, 128), wide)

    def pieces(lv, c):
        slot = lv * ny - 1
        if lv == 0:
            return k_ref.at[:, cols(c)], v_ref.at[:, cols(c)]
        return kbuf.at[slot, :, cols(c)], vbuf.at[slot, :, cols(c)]

    def landing(o, c):
        return kbuf.at[o - 1, :, cols(c)], vbuf.at[o - 1, :, cols(c)]

    def copies(lv, o, c, send, where):
        if c is None:
            src = doc_ref if lv == 0 else docs.at[lv * ny]
            return [remote(src, docs.at[o], send.at[0], recv.at[o, 0], where)]
        out = []
        for j, (src, dst) in enumerate(zip(pieces(lv, c), landing(o, c))):
            p = 1 + 2 * c + j
            out.append(remote(src, dst, send.at[p], recv.at[o, p], where))
        return out

    def z_copies(lv, c):
        return copies(lv, (lv + 1) * ny, c, z_s.at[lv], above)

    def y_copies(lv, d, c):
        other = (y + d) % ny
        return copies(lv, lv * ny + other - y, c, y_s.at[lv, d - 1], (z * ny + other, me))

    def holds(lv):
        return z >= lv

    def y_wanted(lv, d):
        o = lv * ny + (y + d) % ny - y
        return holds(lv) & (o >= 0) & (o <= window)

    def spread(lv, c, act):
        if lv < up:

            @pl.when(holds(lv) & (z < last))
            def _():
                for copy in z_copies(lv, c):
                    act(copy)

        for d in range(1, ny):

            @pl.when(y_wanted(lv, d))
            def _(d=d):
                for copy in y_copies(lv, d, c):
                    act(copy)

    def start(copy):
        copy.start()

    def arrive(o, c):
        @pl.when(seq >= o)
        def _():
            if c is None:
                remote(docs.at[o], docs.at[o], z_s.at[0, 0], recv.at[o, 0], partner).wait_recv()
                return
            for j, dst in enumerate(landing(o, c)):
                p = 1 + 2 * c + j
                remote(dst, dst, z_s.at[0, p], recv.at[o, p], partner).wait_recv()

    spread(0, None, start)
    spread(0, 0, start)
    load_in = pltpu.make_async_copy(win_hbm, win, load_sem.at[0])
    load_in.start()
    load_out = pltpu.make_async_copy(wout_hbm, wout, load_sem.at[1])
    load_out.start()
    load_proj = pltpu.make_async_copy(proj_hbm, proj, load_sem.at[2])
    load_proj.start()
    for o in range(1, window + 1):

        @pl.when(seq < o)
        def _(o=o):
            kbuf[o - 1] = jnp.zeros((rows, width), bf16)
            vbuf[o - 1] = jnp.zeros((rows, width), bf16)
            docs[o] = jnp.full(docs.shape[1:], -1, jnp.int32)

    docs[0] = doc_ref[...]
    arrive(ny, None)
    spread(1, None, start)
    for c in range(1, count):
        spread(0, c, start)

    load_in.wait()
    hidden = win.shape[1]
    picks = (
        lax.broadcasted_iota(jnp.int32, (hidden, slots), 0) == row_ref[...]
    ).astype(f32).astype(bf16)
    step_in = 128

    @pl.loop(0, width // step_in)
    def _(r):
        here = pl.ds(pl.multiple_of(r * step_in, step_in), step_in)
        hot_in[here, :] = jnp.dot(win[here, :], picks, preferred_element_type=f32).astype(bf16)

    load_out.wait()

    @pl.loop(0, slots // BLOCK)
    def _(r):
        here = pl.ds(pl.multiple_of(r * BLOCK, BLOCK), BLOCK)
        chosen = (
            lax.broadcasted_iota(jnp.int32, (BLOCK, hidden), 1) == col_ref[here, :]
        ).astype(f32).astype(bf16)
        hot_out_ref[here, :] = jnp.dot(chosen, wout[...], preferred_element_type=f32).astype(bf16)

    for lv in range(1, up):

        @pl.loop(0, count)
        def _(c, lv=lv):
            arrive(lv * ny, c)
            spread(lv, c, start)

    for lv in range(2, up + 1):
        arrive(lv * ny, None)
        spread(lv, None, start)
    for o in range(1, window + 1):
        if o % ny:
            arrive(o, None)
    row = lax.broadcasted_iota(jnp.int32, (rows, rows), 0)
    col = lax.broadcasted_iota(jnp.int32, (rows, rows), 1)
    for o in range(window + 1):
        seen = qdoc_ref[...] == docs[o, 0:1, :]
        if o == 0:
            seen = seen & (row >= col)
        bias[o] = jnp.where(seen, 0.0, masked_score)

    factor = scale * 1.4426950408889634

    def attend(c):
        for o in range(1, window + 1):
            if o % ny:
                arrive(o, c)
        for h in range(per):
            here = pl.ds(pl.multiple_of(c * wide + h * HEAD_DIM, HEAD_DIM), HEAD_DIM)
            query = q_ref[:, here]
            top = None
            for o in range(window + 1):
                key = k_ref[:, here] if o == 0 else kbuf[o - 1, :, here]
                score = lax.dot_general(
                    query, key, (((1,), (1,)), ((), ())), preferred_element_type=f32
                ) + bias[o]
                scores[h, o] = score
                top = score if top is None else jnp.maximum(top, score)
            peak = jnp.max(top, axis=1, keepdims=True)
            accum = None
            for o in range(window + 1):
                value = v_ref[:, here] if o == 0 else vbuf[o - 1, :, here]
                both = jnp.concatenate([value, jnp.ones((rows, HEAD_DIM), bf16)], axis=1)
                weight = jnp.exp2((scores[h, o] - peak) * factor).astype(bf16)
                term = jnp.dot(weight, both, preferred_element_type=f32)
                accum = term if accum is None else accum + term
            attended[:, here] = (accum[:, :HEAD_DIM] / accum[:, HEAD_DIM:]).astype(bf16)

    @pl.loop(0, count + 1)
    def _(i):
        @pl.when(i < count)
        def _():
            arrive(up * ny, i)
            spread(up, i, start)

        @pl.when(i > 0)
        def _():
            attend(i - 1)

    shared = []
    for d in range(1, ny):
        copy = remote(
            hot_in, all_ref.at[:, pl.ds(d * slots, slots)], w_s.at[d - 1], w_r.at[d - 1],
            (z * ny + (y + ny - d) % ny, me),
        )
        copy.start()
        shared.append(copy)
    own = pltpu.make_async_copy(hot_in, all_ref.at[:, pl.ds(0, slots)], own_sem)
    own.start()
    load_proj.wait()

    parts = far_part.shape[1]
    band = rows // parts

    def block(r, target, side):
        where = pl.ds(pl.multiple_of((target * 2 + side) * width, 128), width)
        return jnp.dot(
            attended[pl.ds(r * band, band), :], proj[:, where], preferred_element_type=f32
        )

    far_copies = []
    for d in range(1, chips):
        for r in range(parts):
            far_part[d - 1, r] = block(r, (chip + d) % chips, 1 - core).astype(bf16)
            copy = remote(
                far_part.at[d - 1, r], far_near.at[d - 1, r], f_s.at[d - 1, r], f_r.at[d - 1, r],
                partner,
            )
            copy.start()
            far_copies.append(copy)
    across = []
    for d in range(1, chips):
        target = (chip + d) % chips
        for r in range(parts):
            mine = block(r, target, core)
            far_copies[(d - 1) * parts + r].wait_recv()
            sums[d - 1, r] = (mine + far_near[d - 1, r].astype(f32)).astype(bf16)
            copy = remote(
                sums.at[d - 1, r], far.at[d - 1, r], x_s.at[d - 1, r], x_r.at[d - 1, r],
                (seq, target * 2 + core),
            )
            copy.start()
            across.append(copy)
    near_copies = []
    for r in range(parts):
        near_part[r] = block(r, chip, 1 - core).astype(bf16)
        copy = remote(near_part.at[r], near_near.at[r], n_s.at[r], n_r.at[r], partner)
        copy.start()
        near_copies.append(copy)
    for r in range(parts):
        here = pl.ds(r * band, band)
        mine = block(r, chip, core)
        near_copies[r].wait_recv()
        total[here, :] = resid_ref[here, :].astype(f32) + (mine + near_near[r].astype(f32))
    lengths = []
    for r in range(parts):
        here = pl.ds(r * band, band)
        value = total[here, :]
        for d in range(1, chips):
            across[(d - 1) * parts + r].wait_recv()
            value = value + far[d - 1, r].astype(f32)
        state = value.astype(bf16)
        state_ref[here, :] = state
        widened = state.astype(f32)
        lengths.append(jnp.sum(widened * widened, axis=1, keepdims=True))
    length = jnp.concatenate(lengths, axis=0)
    flat = jnp.broadcast_to(length, (rows, 128)).T
    squares[me] = flat[0:8, :]
    for d in range(1, nmp):
        remote(
            squares.at[me], squares.at[me], q_s.at[d - 1], q_r.at[me], (seq, (me + d) % nmp)
        ).start()
    for d in range(1, nmp):
        other = (me + d) % nmp
        remote(
            squares.at[other], squares.at[other], q_s.at[d - 1], q_r.at[other], (seq, other)
        ).wait_recv()
    square = squares[0]
    for k in range(1, nmp):
        square = square + squares[k]
    inverse = lax.rsqrt(square / (width * nmp) + epsilon)
    column = jnp.broadcast_to(inverse[0:1, :], (128, rows)).T[:, 0:1]
    for r in range(parts):
        here = pl.ds(r * band, band)
        widened = state_ref[here, :].astype(f32)
        normed_ref[here, :] = (
            widened * column[r * band : (r + 1) * band] * gain_ref[...].astype(f32)
        ).astype(bf16)

    for lv in range(up + 1):
        spread(lv, None, lambda copy: copy.wait_send())

        @pl.loop(0, count)
        def _(c, lv=lv):
            spread(lv, c, lambda copy: copy.wait_send())

    for copy in far_copies + across + near_copies:
        copy.wait_send()
    for d in range(1, nmp):
        remote(
            squares.at[me], squares.at[me], q_s.at[d - 1], q_r.at[me], (seq, (me + d) % nmp)
        ).wait_send()
    for copy in shared:
        copy.wait()
    own.wait()


def front(queries, keys, values, doc_ids, resid, gain, chosen, w_in, w_out, out_proj, ny, collective_id):
    rows, width = queries.shape
    n = lax.axis_size("seq")
    nmp = lax.axis_size("mp")
    nz = n // ny
    chips = nmp // 2
    window = n // 2
    up = min(nz - 1, -(-window // ny))
    heads = width // HEAD_DIM
    per = 2 if heads % 2 == 0 else 1
    pieces = 1 + 2 * (heads // per)
    slots = chosen.shape[0]
    parts = 2
    band = rows // parts
    dma = pltpu.SemaphoreType.DMA
    vmem = pl.BlockSpec(memory_space=VMEM)
    anywhere = pl.BlockSpec(memory_space=pl.ANY)
    f32 = jnp.float32
    bf16 = jnp.bfloat16
    doc_row = jnp.broadcast_to(doc_ids[None, :], (8, rows))
    return pl.pallas_call(
        functools.partial(front_kernel, nz, ny, nmp, up, window, per, HEAD_DIM ** (-0.5)),
        out_shape=[
            jax.ShapeDtypeStruct((rows, width), bf16),
            jax.ShapeDtypeStruct((rows, width), bf16),
            jax.ShapeDtypeStruct((width, ny * slots), bf16),
            jax.ShapeDtypeStruct((slots, width), bf16),
        ],
        in_specs=[vmem] * 9 + [anywhere] * 3,
        out_specs=[vmem, vmem, anywhere, vmem],
        scratch_shapes=[
            VMEM((window, rows, width), bf16),
            VMEM((window, rows, width), bf16),
            VMEM((window + 1, 8, rows), jnp.int32),
            VMEM((window + 1, rows, rows), f32),
            VMEM((per, window + 1, rows, rows), f32),
            VMEM((rows, width), bf16),
            VMEM(out_proj.shape, bf16),
            VMEM(w_in.shape, bf16),
            VMEM(w_out.shape, bf16),
            VMEM((width, slots), bf16),
            VMEM((chips - 1, parts, band, width), bf16),
            VMEM((parts, band, width), bf16),
            VMEM((chips - 1, parts, band, width), bf16),
            VMEM((parts, band, width), bf16),
            VMEM((chips - 1, parts, band, width), bf16),
            VMEM((chips - 1, parts, band, width), bf16),
            VMEM((rows, width), f32),
            VMEM((nmp, 8, rows), f32),
            dma((3,)),
            dma((up, pieces)),
            dma((up + 1, ny - 1, pieces)),
            dma((window + 1, pieces)),
            dma((chips - 1, parts)),
            dma((chips - 1, parts)),
            dma((parts,)),
            dma((parts,)),
            dma((chips - 1, parts)),
            dma((chips - 1, parts)),
            dma((nmp - 1,)),
            dma((nmp,)),
            dma((ny - 1,)),
            dma((ny - 1,)),
            dma,
        ],
        compiler_params=pltpu.CompilerParams(
            collective_id=collective_id, has_side_effects=True, vmem_limit_bytes=63 * 1024 * 1024
        ),
    )(
        queries, keys, values, doc_row, doc_ids[:, None], resid, gain[None, :],
        chosen[None, :], chosen[:, None], w_in, w_out, out_proj,
    )


def ffn_kernel(
    nz, ny, nmp, count, total_tokens,
    x_ref, state_ref, win_ref, wout_ref, out_ref, mean_ref,
    win, wout, gathered, part, own_part, near, pair, active, contrib, moving, from_below, from_above,
    hot, hot_near, hot_send, hot_other,
    load_sem, ag_s, ag_r, pd_s, pd_r, px_s, px_r, ad_s, ad_r, up_s, up_r, dn_s, dn_r, wo_s, wo_r, hp_s, hp_r, hy_s, hy_r,
):
    f32 = jnp.float32
    bf16 = jnp.bfloat16
    seq = lax.axis_index("seq")
    me = lax.axis_index("mp")
    z = seq // ny
    y = seq % ny
    chips = nmp // 2
    chip = me // 2
    core = me % 2
    rows, width = x_ref.shape
    slots = wout_ref.shape[0]
    size = rows // count
    half = nz // 2
    span = half * size
    last = nz - 1
    partner = (seq, chip * 2 + 1 - core)

    def at_z(step):
        return ((z + step) * ny + y, me)

    def at_y(d):
        return (z * ny + (y + d) % ny, me)

    def at_x(d):
        return (seq, ((chip + d) % chips) * 2 + core)

    barrier = pltpu.get_barrier_semaphore()

    def greet(where):
        pl.semaphore_signal(barrier, inc=1, device_id=where, device_id_type=MESH)

    @pl.when(z > 0)
    def _():
        greet(at_z(-1))

    @pl.when(z < last)
    def _():
        greet(at_z(1))

    greet(partner)
    for d in range(1, chips):
        greet(at_x(d))
    for d in range(1, ny):
        greet(at_y(d))
    below = jnp.where(z > 0, 1, 0)
    above = jnp.where(z < last, 1, 0)
    pl.semaphore_wait(barrier, below + above + chips + ny - 1)

    def remote(src, dst, send, recv, where):
        return pltpu.make_async_remote_copy(
            src_ref=src, dst_ref=dst, send_sem=send, recv_sem=recv,
            device_id=where, device_id_type=MESH,
        )

    def own_rows(c):
        return x_ref.at[pl.ds(c * size, size)]

    def gather_copy(step, k, c):
        block = z - step * k
        src = own_rows(c) if k == 0 else gathered.at[c, block]
        way = 0 if step > 0 else 1
        return remote(src, gathered.at[c, block], ag_s.at[way, k, c], ag_r.at[block, c], at_z(step))

    def can_pass(step, k):
        block = z - step * k
        there = z + step
        return (block >= 0) & (block < nz) & (there >= 0) & (there < nz)

    def pass_on(k, c, steps=(1, -1)):
        for step in steps:

            @pl.when(can_pass(step, k))
            def _(step=step):
                gather_copy(step, k, c).start()

    def own_send(c):
        pass_on(0, c)

    def collect(c):
        gathered[c, z] = x_ref[pl.ds(c * size, size), :]
        for k in range(1, nz):
            for step in (1, -1):
                block = z - step * k

                @pl.when((block >= 0) & (block < nz))
                def _(step=step, k=k, block=block):
                    remote(
                        gathered.at[c, block], gathered.at[c, block],
                        ag_s.at[0, 0, c], ag_r.at[block, c], partner,
                    ).wait_recv()
                    if k < nz - 1:
                        pass_on(k, c, (step,))

    def half_rows(side):
        return pl.ds(side * half, half)

    def pre_copy(c):
        return remote(part.at[c], near.at[c], pd_s.at[c], pd_r.at[c], partner)

    def multiply_in(c):
        other = gathered[c, half_rows(1 - core)].reshape(span, width)
        part[c] = jnp.dot(other, win[...], preferred_element_type=f32).astype(bf16)
        pre_copy(c).start()
        mine = gathered[c, half_rows(core)].reshape(span, width)
        own_part[c] = jnp.dot(mine, win[...], preferred_element_type=f32)

    def across_copy(d, c):
        return remote(
            pair.at[c, chip], pair.at[c, chip], px_s.at[d - 1, c], px_r.at[chip, c], at_x(d)
        )

    def exchange(c):
        pre_copy(c).wait_recv()
        pair[c, chip] = (own_part[c] + near[c].astype(f32)).astype(bf16)
        for d in range(1, chips):
            across_copy(d, c).start()

    def active_copy(c):
        return remote(
            active.at[c, half_rows(core)], active.at[c, half_rows(core)],
            ad_s.at[c], ad_r.at[c], partner,
        )

    def activate(c):
        for d in range(1, chips):
            other = (chip + d) % chips
            remote(
                pair.at[c, other], pair.at[c, other], px_s.at[d - 1, c], px_r.at[other, c], at_x(d)
            ).wait_recv()
        pre = pair[c, 0].astype(f32)
        for k in range(1, chips):
            pre = pre + pair[c, k].astype(f32)
        value = jnp.maximum(pre, 0.0)
        active[c, half_rows(core)] = value.astype(bf16).reshape(half, size, value.shape[1])
        active_copy(c).start()
        hot[...] += jnp.sum(value.reshape(span // 8, 8, value.shape[1]), axis=0)

    def up_copy(t, c):
        return remote(moving.at[c, t], from_below.at[c, t], up_s.at[t, c], up_r.at[t, c], at_z(1))

    def down_copy(t, c):
        return remote(moving.at[c, t], from_above.at[c, t], dn_s.at[t, c], dn_r.at[t, c], at_z(-1))

    def multiply_out(c):
        other = half_rows(1 - core)
        remote(active.at[c, other], active.at[c, other], ad_s.at[c], ad_r.at[c], partner).wait_recv()
        lhs = active[c].reshape(nz * size, active.shape[3])
        contrib[c] = jnp.dot(lhs, wout[...], preferred_element_type=f32).reshape(nz, size, width)

        @pl.when(z == 0)
        def _():
            for t in range(last, 0, -1):
                moving[c, t] = contrib[c, t].astype(bf16)
                up_copy(t, c).start()

        @pl.when(z == last)
        def _():
            for t in range(last):
                moving[c, t] = contrib[c, t].astype(bf16)
                down_copy(t, c).start()

    def middle(c):
        for k in range(nz - 1, 0, -1):
            up = z + k

            @pl.when((z > 0) & (up < nz))
            def _(up=up):
                up_copy(up, c).wait_recv()
                moving[c, up] = (contrib[c, up] + from_below[c, up].astype(f32)).astype(bf16)
                up_copy(up, c).start()

            down = z - k

            @pl.when((z < last) & (down >= 0))
            def _(down=down):
                down_copy(down, c).wait_recv()
                moving[c, down] = (contrib[c, down] + from_above[c, down].astype(f32)).astype(bf16)
                down_copy(down, c).start()

    def finish(c):
        @pl.when(z > 0)
        def _():
            up_copy(z, c).wait_recv()
            contrib[c, z] += from_below[c, z].astype(f32)

        @pl.when(z < last)
        def _():
            down_copy(z, c).wait_recv()
            contrib[c, z] += from_above[c, z].astype(f32)

        here = pl.ds(c * size, size)
        out_ref[here, :] = (state_ref[here, :].astype(f32) + contrib[c, z]).astype(bf16)

    def wout_copy(d):
        return remote(
            wout_ref, wout.at[pl.ds(d * slots, slots)], wo_s.at[d - 1], wo_r.at[d - 1], at_y(ny - d)
        )

    own_send(0)
    load_in = pltpu.make_async_copy(win_ref, win, load_sem.at[0])
    load_in.start()
    load_out = pltpu.make_async_copy(wout_ref, wout.at[pl.ds(0, slots)], load_sem.at[1])
    load_out.start()
    for d in range(1, ny):
        wout_copy(d).start()
    own_send(1)
    hot[...] = jnp.zeros_like(hot)
    for i in range(count + 2):
        if i < count:
            collect(i)
            if i + 2 < count:
                own_send(i + 2)
            if i == 0:
                load_in.wait()
            multiply_in(i)
        if 1 <= i <= count:
            activate(i - 1)
        if i < count:
            exchange(i)
        if i == 1:
            load_out.wait()
            for d in range(1, ny):
                wout_copy(d).wait_recv()
        if 1 <= i <= count:
            multiply_out(i - 1)
        if i >= 2:
            middle(i - 2)

    hot_pair = remote(hot, hot_near, hp_s, hp_r, partner)
    hot_pair.start()
    hot_pair.wait_recv()
    both = jnp.sum(hot[...] + hot_near[...], axis=0, keepdims=True)
    hot_send[...] = jnp.broadcast_to(both, hot_send.shape)

    def mean_copy(d):
        return remote(
            hot_send.at[:, pl.ds(d * slots, slots)], hot_other.at[d - 1],
            hy_s.at[d - 1], hy_r.at[d - 1], at_y(d),
        )

    for d in range(1, ny):
        mean_copy(d).start()
    for c in range(count):
        finish(c)
    total = hot_send[0:1, 0:slots]
    for d in range(1, ny):
        mean_copy(d).wait_recv()
        total = total + hot_other[d - 1, 0:1, :]
    mean_ref[...] = total / total_tokens

    for c in range(count):
        for k in range(nz - 1):
            for step in (1, -1):

                @pl.when(can_pass(step, k))
                def _(step=step, k=k, c=c):
                    gather_copy(step, k, c).wait_send()

        pre_copy(c).wait_send()
        for d in range(1, chips):
            across_copy(d, c).wait_send()
        active_copy(c).wait_send()
        for t in range(nz):

            @pl.when((t > z) & (z < last))
            def _(t=t, c=c):
                up_copy(t, c).wait_send()

            @pl.when((t < z) & (z > 0))
            def _(t=t, c=c):
                down_copy(t, c).wait_send()

    for d in range(1, ny):
        wout_copy(d).wait_send()
        mean_copy(d).wait_send()
    hot_pair.wait_send()


def ffn(normed, state, win, wout, ny, count, total_tokens, collective_id):
    rows, width = normed.shape
    slots = wout.shape[0]
    n = lax.axis_size("seq")
    nmp = lax.axis_size("mp")
    nz = n // ny
    chips = nmp // 2
    size = rows // count
    span = (nz // 2) * size
    wide = ny * slots
    dma = pltpu.SemaphoreType.DMA
    vmem = pl.BlockSpec(memory_space=VMEM)
    anywhere = pl.BlockSpec(memory_space=pl.ANY)
    f32 = jnp.float32
    bf16 = jnp.bfloat16
    return pl.pallas_call(
        functools.partial(ffn_kernel, nz, ny, nmp, count, total_tokens),
        out_shape=[
            jax.ShapeDtypeStruct((rows, width), bf16),
            jax.ShapeDtypeStruct((1, slots), f32),
        ],
        in_specs=[vmem, vmem, anywhere, anywhere],
        out_specs=[vmem, vmem],
        scratch_shapes=[
            VMEM((width, wide), bf16),
            VMEM((wide, width), bf16),
            VMEM((count, nz, size, width), bf16),
            VMEM((count, span, wide), bf16),
            VMEM((count, span, wide), f32),
            VMEM((count, span, wide), bf16),
            VMEM((count, chips, span, wide), bf16),
            VMEM((count, nz, size, wide), bf16),
            VMEM((count, nz, size, width), f32),
            VMEM((count, nz, size, width), bf16),
            VMEM((count, nz, size, width), bf16),
            VMEM((count, nz, size, width), bf16),
            VMEM((8, wide), f32),
            VMEM((8, wide), f32),
            VMEM((8, wide), f32),
            VMEM((ny - 1, 8, slots), f32),
            dma((2,)),
            dma((2, nz, count)),
            dma((nz, count)),
            dma((count,)),
            dma((count,)),
            dma((chips - 1, count)),
            dma((chips, count)),
            dma((count,)),
            dma((count,)),
            dma((nz, count)),
            dma((nz, count)),
            dma((nz, count)),
            dma((nz, count)),
            dma((ny - 1,)),
            dma((ny - 1,)),
            dma,
            dma,
            dma((ny - 1,)),
            dma((ny - 1,)),
        ],
        compiler_params=pltpu.CompilerParams(
            collective_id=collective_id, has_side_effects=True, vmem_limit_bytes=60 * 1024 * 1024
        ),
    )(normed, state, win, wout)


def local(
    ny,
    resid,
    queries,
    keys,
    values,
    doc_ids,
    out_proj,
    ffn_gain,
    w_in,
    w_out,
    hot_index,
    hot_blocks,
):
    rows = resid.shape[0]
    total_tokens = rows * lax.axis_size("seq")
    slots = hot_index.shape[1]
    live = jnp.arange(slots, dtype=jnp.int32) < BLOCK * hot_blocks[0]
    chosen = jnp.where(live, hot_index[0], -1)
    state, normed, win, hot_out = front(
        queries, keys, values, doc_ids, resid, ffn_gain, chosen, w_in, w_out, out_proj, ny, 0
    )
    return ffn(normed, state, win, hot_out, ny, 4, total_tokens, 1)


def solution(mesh):
    return jax.shard_map(
        functools.partial(local, row_length(mesh)),
        mesh=mesh,
        in_specs=(
            P("seq", "mp"),
            P("seq", "mp"),
            P("seq", "mp"),
            P("seq", "mp"),
            P("seq"),
            P("mp", None),
            P("mp"),
            P("mp", "seq"),
            P("seq", "mp"),
            P("seq", None),
            P("seq"),
        ),
        out_specs=(P("seq", "mp"), P("seq", None)),
        check_vma=False,
    )
```

```python
import functools

import jax
import jax.numpy as jnp
from jax import lax
from jax.experimental import pallas as pl
from jax.experimental.pallas import tpu as pltpu
from jax.sharding import PartitionSpec as P

HEAD_DIM = 128
BLOCK = 128
MESH = pl.DeviceIdType.MESH
VMEM = pltpu.VMEM

epsilon = 1e-05
masked_score = -1e30


def row_length(mesh):
    seq = mesh.shape["seq"]
    try:
        first = [mesh.devices[i, 0].coords for i in range(seq)]
        size = len({c[1] for c in first})
        if seq % size == 0:
            return size
    except (AttributeError, IndexError, TypeError):
        pass
    return 2


def front_kernel(
    nz, ny, nmp, up, window, per, scale,
    q_ref, k_ref, v_ref, doc_ref, resid_ref, gain_ref, index_ref, live_ref, win_hbm, wout_hbm, proj_hbm,
    state_ref, normed_ref, all_ref, hot_out_ref,
    kbuf, vbuf, docs, bias, scores, attended, proj, win, wout, hot_in,
    far_part, near_part, far_near, near_near, sums, far, total, squares,
    load_sem, z_s, y_s, recv, f_s, f_r, n_s, n_r, x_s, x_r, q_s, q_r, w_s, w_r, own_sem,
):
    f32 = jnp.float32
    bf16 = jnp.bfloat16
    seq = lax.axis_index("seq")
    me = lax.axis_index("mp")
    z = seq // ny
    y = seq % ny
    chips = nmp // 2
    chip = me // 2
    core = me % 2
    rows, width = q_ref.shape
    wide = per * HEAD_DIM
    count = width // wide
    slots = index_ref.shape[1]
    last = nz - 1
    partner = (seq, chip * 2 + 1 - core)

    barrier = pltpu.get_barrier_semaphore()

    def greet(where):
        pl.semaphore_signal(barrier, inc=1, device_id=where, device_id_type=MESH)

    above = ((z + 1) * ny + y, me)

    @pl.when(z > 0)
    def _():
        greet(((z - 1) * ny + y, me))

    @pl.when(z < last)
    def _():
        greet(above)

    for d in range(1, nmp):
        greet((seq, (me + d) % nmp))
    for d in range(1, ny):
        greet((z * ny + (y + d) % ny, me))
    has_below = jnp.where(z > 0, 1, 0)
    has_above = jnp.where(z < last, 1, 0)
    pl.semaphore_wait(barrier, has_below + has_above + nmp + ny - 2)

    def remote(src, dst, send, got, where):
        return pltpu.make_async_remote_copy(
            src_ref=src, dst_ref=dst, send_sem=send, recv_sem=got,
            device_id=where, device_id_type=MESH,
        )

    def cols(c):
        return pl.ds(pl.multiple_of(c * wide, 128), wide)

    def pieces(lv, c):
        slot = lv * ny - 1
        if lv == 0:
            return k_ref.at[:, cols(c)], v_ref.at[:, cols(c)]
        return kbuf.at[slot, :, cols(c)], vbuf.at[slot, :, cols(c)]

    def landing(o, c):
        return kbuf.at[o - 1, :, cols(c)], vbuf.at[o - 1, :, cols(c)]

    def copies(lv, o, c, send, where):
        if c is None:
            src = doc_ref if lv == 0 else docs.at[lv * ny]
            return [remote(src, docs.at[o], send.at[0], recv.at[o, 0], where)]
        out = []
        for j, (src, dst) in enumerate(zip(pieces(lv, c), landing(o, c))):
            p = 1 + 2 * c + j
            out.append(remote(src, dst, send.at[p], recv.at[o, p], where))
        return out

    def z_copies(lv, c):
        return copies(lv, (lv + 1) * ny, c, z_s.at[lv], above)

    def y_copies(lv, d, c):
        other = (y + d) % ny
        return copies(lv, lv * ny + other - y, c, y_s.at[lv, d - 1], (z * ny + other, me))

    def holds(lv):
        return z >= lv

    def y_wanted(lv, d):
        o = lv * ny + (y + d) % ny - y
        return holds(lv) & (o >= 0) & (o <= window)

    def spread(lv, c, act):
        if lv < up:

            @pl.when(holds(lv) & (z < last))
            def _():
                for copy in z_copies(lv, c):
                    act(copy)

        for d in range(1, ny):

            @pl.when(y_wanted(lv, d))
            def _(d=d):
                for copy in y_copies(lv, d, c):
                    act(copy)

    def start(copy):
        copy.start()

    def arrive(o, c):
        @pl.when(seq >= o)
        def _():
            if c is None:
                remote(docs.at[o], docs.at[o], z_s.at[0, 0], recv.at[o, 0], partner).wait_recv()
                return
            for j, dst in enumerate(landing(o, c)):
                p = 1 + 2 * c + j
                remote(dst, dst, z_s.at[0, p], recv.at[o, p], partner).wait_recv()

    spread(0, None, start)
    spread(0, 0, start)
    load_in = pltpu.make_async_copy(win_hbm, win, load_sem.at[0])
    load_in.start()
    load_out = pltpu.make_async_copy(wout_hbm, wout, load_sem.at[1])
    load_out.start()
    load_proj = pltpu.make_async_copy(proj_hbm, proj, load_sem.at[2])
    load_proj.start()
    for o in range(1, window + 1):

        @pl.when(seq < o)
        def _(o=o):
            kbuf[o - 1] = jnp.zeros((rows, width), bf16)
            vbuf[o - 1] = jnp.zeros((rows, width), bf16)
            docs[o] = jnp.full(docs.shape[1:], -1, jnp.int32)

    docs[0] = doc_ref[...]
    arrive(ny, None)
    spread(1, None, start)
    for c in range(1, count):
        spread(0, c, start)

    load_in.wait()
    hidden = win.shape[0]
    order = lax.broadcasted_iota(jnp.int32, (1, slots), 1)
    chosen = jnp.where(order < BLOCK * live_ref[0], index_ref[...], -1).astype(f32)
    chosen = jnp.broadcast_to(chosen, (BLOCK, slots))
    neurons = lax.broadcasted_iota(jnp.int32, (BLOCK, hidden), 1).astype(f32)

    def picked(r, weights):
        here = slice(r * BLOCK, (r + 1) * BLOCK)
        picks = (neurons == chosen[:, here].T[:, 0:1]).astype(f32).astype(bf16)
        return jnp.dot(picks, weights[...], preferred_element_type=f32)

    for r in range(slots // BLOCK):
        hot_in[:, r * BLOCK : (r + 1) * BLOCK] = picked(r, win).T.astype(bf16)
    load_out.wait()
    for r in range(slots // BLOCK):
        hot_out_ref[r * BLOCK : (r + 1) * BLOCK, :] = picked(r, wout).astype(bf16)

    for lv in range(1, up):

        @pl.loop(0, count)
        def _(c, lv=lv):
            arrive(lv * ny, c)
            spread(lv, c, start)

    for lv in range(2, up + 1):
        arrive(lv * ny, None)
        spread(lv, None, start)
    for o in range(1, window + 1):
        if o % ny:
            arrive(o, None)
    row = lax.broadcasted_iota(jnp.int32, (rows, rows), 0)
    col = lax.broadcasted_iota(jnp.int32, (rows, rows), 1)
    mine = jnp.broadcast_to(doc_ref[...].astype(f32), (128, rows)).T[:, 0:1]
    for o in range(window + 1):
        seen = mine == docs[o].astype(f32)
        if o == 0:
            seen = seen & (row >= col)
        bias[o] = jnp.where(seen, 0.0, masked_score)

    factor = scale * 1.4426950408889634

    def attend(c):
        for o in range(1, window + 1):
            if o % ny:
                arrive(o, c)
        for h in range(per):
            here = pl.ds(pl.multiple_of(c * wide + h * HEAD_DIM, HEAD_DIM), HEAD_DIM)
            query = q_ref[:, here]
            top = None
            for o in range(window + 1):
                key = k_ref[:, here] if o == 0 else kbuf[o - 1, :, here]
                score = lax.dot_general(
                    query, key, (((1,), (1,)), ((), ())), preferred_element_type=f32
                ) + bias[o]
                scores[h, o] = score
                top = score if top is None else jnp.maximum(top, score)
            peak = jnp.max(top, axis=1, keepdims=True)
            accum = None
            for o in range(window + 1):
                value = v_ref[:, here] if o == 0 else vbuf[o - 1, :, here]
                both = jnp.concatenate([value, jnp.ones((rows, HEAD_DIM), bf16)], axis=1)
                weight = jnp.exp2((scores[h, o] - peak) * factor).astype(bf16)
                term = jnp.dot(weight, both, preferred_element_type=f32)
                accum = term if accum is None else accum + term
            attended[:, here] = (accum[:, :HEAD_DIM] / accum[:, HEAD_DIM:]).astype(bf16)

    shared = []
    for d in range(1, ny):
        shared.append(remote(
            hot_in, all_ref.at[:, pl.ds(d * slots, slots)], w_s.at[d - 1], w_r.at[d - 1],
            (z * ny + (y + ny - d) % ny, me),
        ))

    @pl.loop(0, count + 1)
    def _(i):
        @pl.when(i < count)
        def _():
            arrive(up * ny, i)
            spread(up, i, start)

        @pl.when(i == count - 1)
        def _():
            for copy in shared:
                copy.start()

        @pl.when(i > 0)
        def _():
            attend(i - 1)

    own = pltpu.make_async_copy(hot_in, all_ref.at[:, pl.ds(0, slots)], own_sem)
    own.start()
    load_proj.wait()

    parts = far_part.shape[1]
    band = rows // parts

    def block(r, target, side):
        where = pl.ds(pl.multiple_of((target * 2 + side) * width, 128), width)
        return jnp.dot(
            attended[pl.ds(r * band, band), :], proj[:, where], preferred_element_type=f32
        )

    far_copies = []
    for d in range(1, chips):
        for r in range(parts):
            far_part[d - 1, r] = block(r, (chip + d) % chips, 1 - core).astype(bf16)
            copy = remote(
                far_part.at[d - 1, r], far_near.at[d - 1, r], f_s.at[d - 1, r], f_r.at[d - 1, r],
                partner,
            )
            copy.start()
            far_copies.append(copy)
    across = []
    for d in range(1, chips):
        target = (chip + d) % chips
        for r in range(parts):
            mine = block(r, target, core)
            far_copies[(d - 1) * parts + r].wait_recv()
            sums[d - 1, r] = (mine + far_near[d - 1, r].astype(f32)).astype(bf16)
            copy = remote(
                sums.at[d - 1, r], far.at[d - 1, r], x_s.at[d - 1, r], x_r.at[d - 1, r],
                (seq, target * 2 + core),
            )
            copy.start()
            across.append(copy)
    near_copies = []
    for r in range(parts):
        near_part[r] = block(r, chip, 1 - core).astype(bf16)
        copy = remote(near_part.at[r], near_near.at[r], n_s.at[r], n_r.at[r], partner)
        copy.start()
        near_copies.append(copy)
    for r in range(parts):
        here = pl.ds(r * band, band)
        mine = block(r, chip, core)
        near_copies[r].wait_recv()
        total[here, :] = resid_ref[here, :].astype(f32) + (mine + near_near[r].astype(f32))
    lengths = []
    for r in range(parts):
        here = pl.ds(r * band, band)
        value = total[here, :]
        for d in range(1, chips):
            across[(d - 1) * parts + r].wait_recv()
            value = value + far[d - 1, r].astype(f32)
        state = value.astype(bf16)
        state_ref[here, :] = state
        widened = state.astype(f32)
        lengths.append(jnp.sum(widened * widened, axis=1, keepdims=True))
    length = jnp.concatenate(lengths, axis=0)
    flat = jnp.broadcast_to(length, (rows, 128)).T
    squares[me] = flat[0:8, :]
    for d in range(1, nmp):
        remote(
            squares.at[me], squares.at[me], q_s.at[d - 1], q_r.at[me], (seq, (me + d) % nmp)
        ).start()
    for d in range(1, nmp):
        other = (me + d) % nmp
        remote(
            squares.at[other], squares.at[other], q_s.at[d - 1], q_r.at[other], (seq, other)
        ).wait_recv()
    square = squares[0]
    for k in range(1, nmp):
        square = square + squares[k]
    inverse = lax.rsqrt(square / (width * nmp) + epsilon)
    column = jnp.broadcast_to(inverse[0:1, :], (128, rows)).T[:, 0:1]
    for r in range(parts):
        here = pl.ds(r * band, band)
        widened = state_ref[here, :].astype(f32)
        normed_ref[here, :] = (
            widened * column[r * band : (r + 1) * band] * gain_ref[...].astype(f32)
        ).astype(bf16)

    for lv in range(up + 1):
        spread(lv, None, lambda copy: copy.wait_send())

        @pl.loop(0, count)
        def _(c, lv=lv):
            spread(lv, c, lambda copy: copy.wait_send())

    for copy in far_copies + across + near_copies:
        copy.wait_send()
    for d in range(1, nmp):
        remote(
            squares.at[me], squares.at[me], q_s.at[d - 1], q_r.at[me], (seq, (me + d) % nmp)
        ).wait_send()
    for copy in shared:
        copy.wait()
    own.wait()


def front(queries, keys, values, doc_ids, resid, gain, index, live, w_in, w_out, out_proj, ny, collective_id):
    rows, width = queries.shape
    n = lax.axis_size("seq")
    nmp = lax.axis_size("mp")
    nz = n // ny
    chips = nmp // 2
    window = n // 2
    up = min(nz - 1, -(-window // ny))
    heads = width // HEAD_DIM
    per = 2 if heads % 2 == 0 else 1
    pieces = 1 + 2 * (heads // per)
    slots = index.shape[1]
    parts = 2
    band = rows // parts
    dma = pltpu.SemaphoreType.DMA
    vmem = pl.BlockSpec(memory_space=VMEM)
    anywhere = pl.BlockSpec(memory_space=pl.ANY)
    f32 = jnp.float32
    bf16 = jnp.bfloat16
    return pl.pallas_call(
        functools.partial(front_kernel, nz, ny, nmp, up, window, per, HEAD_DIM ** (-0.5)),
        out_shape=[
            jax.ShapeDtypeStruct((rows, width), bf16),
            jax.ShapeDtypeStruct((rows, width), bf16),
            jax.ShapeDtypeStruct((width, ny * slots), bf16),
            jax.ShapeDtypeStruct((slots, width), bf16),
        ],
        in_specs=[vmem] * 7 + [pl.BlockSpec(memory_space=pltpu.SMEM)] + [anywhere] * 3,
        out_specs=[vmem, vmem, anywhere, vmem],
        scratch_shapes=[
            VMEM((window, rows, width), bf16),
            VMEM((window, rows, width), bf16),
            VMEM((window + 1, 1, rows), jnp.int32),
            VMEM((window + 1, rows, rows), f32),
            VMEM((per, window + 1, rows, rows), f32),
            VMEM((rows, width), bf16),
            VMEM(out_proj.shape, bf16),
            VMEM(w_in.shape[::-1], bf16),
            VMEM(w_out.shape, bf16),
            VMEM((width, slots), bf16),
            VMEM((chips - 1, parts, band, width), bf16),
            VMEM((parts, band, width), bf16),
            VMEM((chips - 1, parts, band, width), bf16),
            VMEM((parts, band, width), bf16),
            VMEM((chips - 1, parts, band, width), bf16),
            VMEM((chips - 1, parts, band, width), bf16),
            VMEM((rows, width), f32),
            VMEM((nmp, 8, rows), f32),
            dma((3,)),
            dma((up, pieces)),
            dma((up + 1, ny - 1, pieces)),
            dma((window + 1, pieces)),
            dma((chips - 1, parts)),
            dma((chips - 1, parts)),
            dma((parts,)),
            dma((parts,)),
            dma((chips - 1, parts)),
            dma((chips - 1, parts)),
            dma((nmp - 1,)),
            dma((nmp,)),
            dma((ny - 1,)),
            dma((ny - 1,)),
            dma,
        ],
        compiler_params=pltpu.CompilerParams(
            collective_id=collective_id, has_side_effects=True, vmem_limit_bytes=63 * 1024 * 1024
        ),
    )(
        queries, keys, values, doc_ids[None, :], resid, gain[None, :], index, live, w_in.T, w_out, out_proj,
    )


def ffn_kernel(
    nz, ny, nmp, count, total_tokens,
    x_ref, state_ref, win_ref, wout_ref, out_ref, mean_ref,
    win, wout, gathered, part, own_part, near, pair, active, contrib, moving, from_below, from_above,
    hot, hot_near, hot_send, hot_other,
    load_sem, ag_s, ag_r, pd_s, pd_r, px_s, px_r, ad_s, ad_r, up_s, up_r, dn_s, dn_r, wo_s, wo_r, hp_s, hp_r, hy_s, hy_r,
):
    f32 = jnp.float32
    bf16 = jnp.bfloat16
    seq = lax.axis_index("seq")
    me = lax.axis_index("mp")
    z = seq // ny
    y = seq % ny
    chips = nmp // 2
    chip = me // 2
    core = me % 2
    rows, width = x_ref.shape
    slots = wout_ref.shape[0]
    size = rows // count
    half = nz // 2
    span = half * size
    last = nz - 1
    partner = (seq, chip * 2 + 1 - core)

    def at_z(step):
        return ((z + step) * ny + y, me)

    def at_y(d):
        return (z * ny + (y + d) % ny, me)

    def at_x(d):
        return (seq, ((chip + d) % chips) * 2 + core)

    barrier = pltpu.get_barrier_semaphore()

    def greet(where):
        pl.semaphore_signal(barrier, inc=1, device_id=where, device_id_type=MESH)

    @pl.when(z > 0)
    def _():
        greet(at_z(-1))

    @pl.when(z < last)
    def _():
        greet(at_z(1))

    greet(partner)
    for d in range(1, chips):
        greet(at_x(d))
    for d in range(1, ny):
        greet(at_y(d))
    below = jnp.where(z > 0, 1, 0)
    above = jnp.where(z < last, 1, 0)
    pl.semaphore_wait(barrier, below + above + chips + ny - 1)

    def remote(src, dst, send, recv, where):
        return pltpu.make_async_remote_copy(
            src_ref=src, dst_ref=dst, send_sem=send, recv_sem=recv,
            device_id=where, device_id_type=MESH,
        )

    def own_rows(c):
        return x_ref.at[pl.ds(c * size, size)]

    def gather_copy(step, k, c):
        block = z - step * k
        src = own_rows(c) if k == 0 else gathered.at[c, block]
        way = 0 if step > 0 else 1
        return remote(src, gathered.at[c, block], ag_s.at[way, k, c], ag_r.at[block, c], at_z(step))

    def can_pass(step, k):
        block = z - step * k
        there = z + step
        return (block >= 0) & (block < nz) & (there >= 0) & (there < nz)

    def pass_on(k, c, steps=(1, -1)):
        for step in steps:

            @pl.when(can_pass(step, k))
            def _(step=step):
                gather_copy(step, k, c).start()

    def own_send(c):
        pass_on(0, c)

    def collect(c):
        gathered[c, z] = x_ref[pl.ds(c * size, size), :]
        for k in range(1, nz):
            for step in (1, -1):
                block = z - step * k

                @pl.when((block >= 0) & (block < nz))
                def _(step=step, k=k, block=block):
                    remote(
                        gathered.at[c, block], gathered.at[c, block],
                        ag_s.at[0, 0, c], ag_r.at[block, c], partner,
                    ).wait_recv()
                    if k < nz - 1:
                        pass_on(k, c, (step,))

    def half_rows(side):
        return pl.ds(side * half, half)

    def pre_copy(c):
        return remote(part.at[c], near.at[c], pd_s.at[c], pd_r.at[c], partner)

    def multiply_in(c):
        other = gathered[c, half_rows(1 - core)].reshape(span, width)
        part[c] = jnp.dot(other, win[...], preferred_element_type=f32).astype(bf16)
        pre_copy(c).start()
        mine = gathered[c, half_rows(core)].reshape(span, width)
        own_part[c] = jnp.dot(mine, win[...], preferred_element_type=f32)

    def across_copy(d, c):
        return remote(
            pair.at[c, chip], pair.at[c, chip], px_s.at[d - 1, c], px_r.at[chip, c], at_x(d)
        )

    def exchange(c):
        pre_copy(c).wait_recv()
        pair[c, chip] = (own_part[c] + near[c].astype(f32)).astype(bf16)
        for d in range(1, chips):
            across_copy(d, c).start()

    def active_copy(c):
        return remote(
            active.at[c, half_rows(core)], active.at[c, half_rows(core)],
            ad_s.at[c], ad_r.at[c], partner,
        )

    def activate(c):
        for d in range(1, chips):
            other = (chip + d) % chips
            remote(
                pair.at[c, other], pair.at[c, other], px_s.at[d - 1, c], px_r.at[other, c], at_x(d)
            ).wait_recv()
        pre = pair[c, 0].astype(f32)
        for k in range(1, chips):
            pre = pre + pair[c, k].astype(f32)
        value = jnp.maximum(pre, 0.0)
        active[c, half_rows(core)] = value.astype(bf16).reshape(half, size, value.shape[1])
        active_copy(c).start()
        hot[...] += jnp.sum(value.reshape(span // 8, 8, value.shape[1]), axis=0)

    def up_copy(t, c):
        return remote(moving.at[c, t], from_below.at[c, t], up_s.at[t, c], up_r.at[t, c], at_z(1))

    def down_copy(t, c):
        return remote(moving.at[c, t], from_above.at[c, t], dn_s.at[t, c], dn_r.at[t, c], at_z(-1))

    def multiply_out(c):
        other = half_rows(1 - core)
        remote(active.at[c, other], active.at[c, other], ad_s.at[c], ad_r.at[c], partner).wait_recv()
        lhs = active[c].reshape(nz * size, active.shape[3])
        contrib[c] = jnp.dot(lhs, wout[...], preferred_element_type=f32).reshape(nz, size, width)

        @pl.when(z == 0)
        def _():
            for t in range(last, 0, -1):
                moving[c, t] = contrib[c, t].astype(bf16)
                up_copy(t, c).start()

        @pl.when(z == last)
        def _():
            for t in range(last):
                moving[c, t] = contrib[c, t].astype(bf16)
                down_copy(t, c).start()

    def middle(c):
        for k in range(nz - 1, 0, -1):
            up = z + k

            @pl.when((z > 0) & (up < nz))
            def _(up=up):
                up_copy(up, c).wait_recv()
                moving[c, up] = (contrib[c, up] + from_below[c, up].astype(f32)).astype(bf16)
                up_copy(up, c).start()

            down = z - k

            @pl.when((z < last) & (down >= 0))
            def _(down=down):
                down_copy(down, c).wait_recv()
                moving[c, down] = (contrib[c, down] + from_above[c, down].astype(f32)).astype(bf16)
                down_copy(down, c).start()

    def finish(c):
        @pl.when(z > 0)
        def _():
            up_copy(z, c).wait_recv()
            contrib[c, z] += from_below[c, z].astype(f32)

        @pl.when(z < last)
        def _():
            down_copy(z, c).wait_recv()
            contrib[c, z] += from_above[c, z].astype(f32)

        here = pl.ds(c * size, size)
        out_ref[here, :] = (state_ref[here, :].astype(f32) + contrib[c, z]).astype(bf16)

    def wout_copy(d):
        return remote(
            wout_ref, wout.at[pl.ds(d * slots, slots)], wo_s.at[d - 1], wo_r.at[d - 1], at_y(ny - d)
        )

    own_send(0)
    load_in = pltpu.make_async_copy(win_ref, win, load_sem.at[0])
    load_in.start()
    load_out = pltpu.make_async_copy(wout_ref, wout.at[pl.ds(0, slots)], load_sem.at[1])
    load_out.start()
    for d in range(1, ny):
        wout_copy(d).start()
    own_send(1)
    hot[...] = jnp.zeros_like(hot)
    for i in range(count + 2):
        if i < count:
            collect(i)
            if i + 2 < count:
                own_send(i + 2)
            if i == 0:
                load_in.wait()
            multiply_in(i)
        if 1 <= i <= count:
            activate(i - 1)
        if i < count:
            exchange(i)
        if i == 1:
            load_out.wait()
            for d in range(1, ny):
                wout_copy(d).wait_recv()
        if 1 <= i <= count:
            multiply_out(i - 1)
        if i >= 2:
            middle(i - 2)

    hot_pair = remote(hot, hot_near, hp_s, hp_r, partner)
    hot_pair.start()
    hot_pair.wait_recv()
    both = jnp.sum(hot[...] + hot_near[...], axis=0, keepdims=True)
    hot_send[...] = jnp.broadcast_to(both, hot_send.shape)

    def mean_copy(d):
        return remote(
            hot_send.at[:, pl.ds(d * slots, slots)], hot_other.at[d - 1],
            hy_s.at[d - 1], hy_r.at[d - 1], at_y(d),
        )

    for d in range(1, ny):
        mean_copy(d).start()
    for c in range(count):
        finish(c)
    total = hot_send[0:1, 0:slots]
    for d in range(1, ny):
        mean_copy(d).wait_recv()
        total = total + hot_other[d - 1, 0:1, :]
    mean_ref[...] = total / total_tokens

    for c in range(count):
        for k in range(nz - 1):
            for step in (1, -1):

                @pl.when(can_pass(step, k))
                def _(step=step, k=k, c=c):
                    gather_copy(step, k, c).wait_send()

        pre_copy(c).wait_send()
        for d in range(1, chips):
            across_copy(d, c).wait_send()
        active_copy(c).wait_send()
        for t in range(nz):

            @pl.when((t > z) & (z < last))
            def _(t=t, c=c):
                up_copy(t, c).wait_send()

            @pl.when((t < z) & (z > 0))
            def _(t=t, c=c):
                down_copy(t, c).wait_send()

    for d in range(1, ny):
        wout_copy(d).wait_send()
        mean_copy(d).wait_send()
    hot_pair.wait_send()


def ffn(normed, state, win, wout, ny, count, total_tokens, collective_id):
    rows, width = normed.shape
    slots = wout.shape[0]
    n = lax.axis_size("seq")
    nmp = lax.axis_size("mp")
    nz = n // ny
    chips = nmp // 2
    size = rows // count
    span = (nz // 2) * size
    wide = ny * slots
    dma = pltpu.SemaphoreType.DMA
    vmem = pl.BlockSpec(memory_space=VMEM)
    anywhere = pl.BlockSpec(memory_space=pl.ANY)
    f32 = jnp.float32
    bf16 = jnp.bfloat16
    return pl.pallas_call(
        functools.partial(ffn_kernel, nz, ny, nmp, count, total_tokens),
        out_shape=[
            jax.ShapeDtypeStruct((rows, width), bf16),
            jax.ShapeDtypeStruct((1, slots), f32),
        ],
        in_specs=[vmem, vmem, anywhere, anywhere],
        out_specs=[vmem, vmem],
        scratch_shapes=[
            VMEM((width, wide), bf16),
            VMEM((wide, width), bf16),
            VMEM((count, nz, size, width), bf16),
            VMEM((count, span, wide), bf16),
            VMEM((count, span, wide), f32),
            VMEM((count, span, wide), bf16),
            VMEM((count, chips, span, wide), bf16),
            VMEM((count, nz, size, wide), bf16),
            VMEM((count, nz, size, width), f32),
            VMEM((count, nz, size, width), bf16),
            VMEM((count, nz, size, width), bf16),
            VMEM((count, nz, size, width), bf16),
            VMEM((8, wide), f32),
            VMEM((8, wide), f32),
            VMEM((8, wide), f32),
            VMEM((ny - 1, 8, slots), f32),
            dma((2,)),
            dma((2, nz, count)),
            dma((nz, count)),
            dma((count,)),
            dma((count,)),
            dma((chips - 1, count)),
            dma((chips, count)),
            dma((count,)),
            dma((count,)),
            dma((nz, count)),
            dma((nz, count)),
            dma((nz, count)),
            dma((nz, count)),
            dma((ny - 1,)),
            dma((ny - 1,)),
            dma,
            dma,
            dma((ny - 1,)),
            dma((ny - 1,)),
        ],
        compiler_params=pltpu.CompilerParams(
            collective_id=collective_id, has_side_effects=True, vmem_limit_bytes=60 * 1024 * 1024
        ),
    )(normed, state, win, wout)


def local(
    ny,
    resid,
    queries,
    keys,
    values,
    doc_ids,
    out_proj,
    ffn_gain,
    w_in,
    w_out,
    hot_index,
    hot_blocks,
):
    rows = resid.shape[0]
    total_tokens = rows * lax.axis_size("seq")
    state, normed, win, hot_out = front(
        queries, keys, values, doc_ids, resid, ffn_gain, hot_index, hot_blocks, w_in, w_out, out_proj, ny, 0
    )
    return ffn(normed, state, win, hot_out, ny, 4, total_tokens, 1)


def solution(mesh):
    return jax.shard_map(
        functools.partial(local, row_length(mesh)),
        mesh=mesh,
        in_specs=(
            P("seq", "mp"),
            P("seq", "mp"),
            P("seq", "mp"),
            P("seq", "mp"),
            P("seq"),
            P("mp", None),
            P("mp"),
            P("mp", "seq"),
            P("seq", "mp"),
            P("seq", None),
            P("seq"),
        ),
        out_specs=(P("seq", "mp"), P("seq", None)),
        check_vma=False,
    )
```

```python
import functools

import jax
import jax.numpy as jnp
from jax import lax
from jax.experimental import pallas as pl
from jax.experimental.pallas import tpu as pltpu
from jax.sharding import PartitionSpec as P

HEAD_DIM = 128
BLOCK = 128
MESH = pl.DeviceIdType.MESH
VMEM = pltpu.VMEM

epsilon = 1e-05
masked_score = -1e30


def row_length(mesh):
    seq = mesh.shape["seq"]
    try:
        first = [mesh.devices[i, 0].coords for i in range(seq)]
        size = len({c[1] for c in first})
        if seq % size == 0:
            return size
    except (AttributeError, IndexError, TypeError):
        pass
    return 2


def ffn_order(nz, count):
    period = 42.0 / count
    timed = []

    def put(at, stage, distance=0):
        for c in range(count):
            timed.append((at + period * c, len(timed), stage, distance, c))

    put(-16.3, "own")
    for k in range(1, nz):
        put(-5.0 + 4.5 * k, "collect", k)
    arrived = -5.0 + 4.5 * (nz - 1)
    put(arrived, "multiply_in")
    put(11.7, "exchange")
    put(18.4, "activate")
    put(22.1, "multiply_out")
    for k in range(nz - 1, 0, -1):
        put(max(38.5 - 4.5 * k, 22.1) if k < nz - 1 else 22.1, "middle", k)
    put(1000.0, "finish")
    return [entry[2:] for entry in sorted(timed)]


def layer_kernel(
    nz, ny, nmp, up, window, per, count, scale, total_tokens,
    q_ref, k_ref, v_ref, doc_ref, resid_ref, gain_ref, index_ref, live_ref, win_hbm, wout_hbm, proj_hbm,
    out_ref, mean_ref,
    kbuf, vbuf, docs, bias, scores, attended, proj, weights, win, wout,
    far_part, far_near, sums, far, near_part, near_near, total, squares, state, normed,
    gathered, part, own_part, near, pair, active, contrib, from_below, from_above,
    hot, hot_near, hot_send, hot_other,
    load_sem, z_s, y_s, recv, f_s, f_r, near_s, near_r, x_s, x_r, q_s, q_r, wi_s, wi_r, wo_s, wo_r,
    ag_s, ag_r, pd_s, pd_r, px_s, px_r, ad_s, ad_r, up_s, up_r, dn_s, dn_r, hp_s, hp_r, hy_s, hy_r,
):
    f32 = jnp.float32
    bf16 = jnp.bfloat16
    seq = lax.axis_index("seq")
    me = lax.axis_index("mp")
    z = seq // ny
    y = seq % ny
    chips = nmp // 2
    chip = me // 2
    core = me % 2
    rows, width = q_ref.shape
    wide = per * HEAD_DIM
    groups = width // wide
    slots = index_ref.shape[1]
    last = nz - 1
    partner = (seq, chip * 2 + 1 - core)

    barrier = pltpu.get_barrier_semaphore()

    def greet(where):
        pl.semaphore_signal(barrier, inc=1, device_id=where, device_id_type=MESH)

    above = ((z + 1) * ny + y, me)

    @pl.when(z > 0)
    def _():
        greet(((z - 1) * ny + y, me))

    @pl.when(z < last)
    def _():
        greet(above)

    for d in range(1, nmp):
        greet((seq, (me + d) % nmp))
    for d in range(1, ny):
        greet((z * ny + (y + d) % ny, me))
    has_below = jnp.where(z > 0, 1, 0)
    has_above = jnp.where(z < last, 1, 0)
    pl.semaphore_wait(barrier, has_below + has_above + nmp + ny - 2)

    def remote(src, dst, send, got, where):
        return pltpu.make_async_remote_copy(
            src_ref=src, dst_ref=dst, send_sem=send, recv_sem=got,
            device_id=where, device_id_type=MESH,
        )

    def cols(c):
        return pl.ds(pl.multiple_of(c * wide, 128), wide)

    def pieces(lv, c):
        slot = lv * ny - 1
        if lv == 0:
            return k_ref.at[:, cols(c)], v_ref.at[:, cols(c)]
        return kbuf.at[slot, :, cols(c)], vbuf.at[slot, :, cols(c)]

    def landing(o, c):
        return kbuf.at[o - 1, :, cols(c)], vbuf.at[o - 1, :, cols(c)]

    def copies(lv, o, c, send, where):
        if c is None:
            src = doc_ref if lv == 0 else docs.at[lv * ny]
            return [remote(src, docs.at[o], send.at[0], recv.at[o, 0], where)]
        out = []
        for j, (src, dst) in enumerate(zip(pieces(lv, c), landing(o, c))):
            p = 1 + 2 * c + j
            out.append(remote(src, dst, send.at[p], recv.at[o, p], where))
        return out

    def z_copies(lv, c):
        return copies(lv, (lv + 1) * ny, c, z_s.at[lv], above)

    def y_copies(lv, d, c):
        other = (y + d) % ny
        return copies(lv, lv * ny + other - y, c, y_s.at[lv, d - 1], (z * ny + other, me))

    def holds(lv):
        return z >= lv

    def y_wanted(lv, d):
        o = lv * ny + (y + d) % ny - y
        return holds(lv) & (o >= 0) & (o <= window)

    def spread(lv, c, act):
        if lv < up:

            @pl.when(holds(lv) & (z < last))
            def _():
                for copy in z_copies(lv, c):
                    act(copy)

        for d in range(1, ny):

            @pl.when(y_wanted(lv, d))
            def _(d=d):
                for copy in y_copies(lv, d, c):
                    act(copy)

    def start(copy):
        copy.start()

    def arrive(o, c):
        @pl.when(seq >= o)
        def _():
            if c is None:
                remote(docs.at[o], docs.at[o], z_s.at[0, 0], recv.at[o, 0], partner).wait_recv()
                return
            for j, dst in enumerate(landing(o, c)):
                p = 1 + 2 * c + j
                remote(dst, dst, z_s.at[0, p], recv.at[o, p], partner).wait_recv()

    spread(0, None, start)
    spread(0, 0, start)
    load_in = pltpu.make_async_copy(win_hbm, weights, load_sem.at[0])
    load_in.start()
    load_proj = pltpu.make_async_copy(proj_hbm, proj, load_sem.at[2])
    load_proj.start()
    for o in range(1, window + 1):

        @pl.when(seq < o)
        def _(o=o):
            kbuf[o - 1] = jnp.zeros((rows, width), bf16)
            vbuf[o - 1] = jnp.zeros((rows, width), bf16)
            docs[o] = jnp.full(docs.shape[1:], -1, jnp.int32)

    docs[0] = doc_ref[...]
    arrive(ny, None)
    spread(1, None, start)
    for c in range(1, groups):
        spread(0, c, start)

    load_in.wait()
    hidden = weights.shape[0]
    order = lax.broadcasted_iota(jnp.int32, (1, slots), 1)
    chosen = jnp.where(order < BLOCK * live_ref[0], index_ref[...], -1).astype(f32)
    chosen = jnp.broadcast_to(chosen, (BLOCK, slots))
    neurons = lax.broadcasted_iota(jnp.int32, (BLOCK, hidden), 1).astype(f32)

    def picked(r):
        here = slice(r * BLOCK, (r + 1) * BLOCK)
        picks = (neurons == chosen[:, here].T[:, 0:1]).astype(f32).astype(bf16)
        return jnp.dot(picks, weights[...], preferred_element_type=f32)

    for r in range(slots // BLOCK):
        win[:, r * BLOCK : (r + 1) * BLOCK] = picked(r).T.astype(bf16)
    load_out = pltpu.make_async_copy(wout_hbm, weights, load_sem.at[1])
    load_out.start()
    load_out.wait()
    for r in range(slots // BLOCK):
        wout[r * BLOCK : (r + 1) * BLOCK, :] = picked(r).astype(bf16)

    for lv in range(1, up):

        @pl.loop(0, groups)
        def _(c, lv=lv):
            arrive(lv * ny, c)
            spread(lv, c, start)

    for lv in range(2, up + 1):
        arrive(lv * ny, None)
        spread(lv, None, start)
    for o in range(1, window + 1):
        if o % ny:
            arrive(o, None)
    row = lax.broadcasted_iota(jnp.int32, (rows, rows), 0)
    col = lax.broadcasted_iota(jnp.int32, (rows, rows), 1)
    mine = jnp.broadcast_to(doc_ref[...].astype(f32), (128, rows)).T[:, 0:1]
    for o in range(window + 1):
        seen = mine == docs[o].astype(f32)
        if o == 0:
            seen = seen & (row >= col)
        bias[o] = jnp.where(seen, 0.0, masked_score)

    factor = scale * 1.4426950408889634

    def attend(c):
        for o in range(1, window + 1):
            if o % ny:
                arrive(o, c)
        for h in range(per):
            here = pl.ds(pl.multiple_of(c * wide + h * HEAD_DIM, HEAD_DIM), HEAD_DIM)
            query = q_ref[:, here]
            top = None
            for o in range(window + 1):
                key = k_ref[:, here] if o == 0 else kbuf[o - 1, :, here]
                score = lax.dot_general(
                    query, key, (((1,), (1,)), ((), ())), preferred_element_type=f32
                ) + bias[o]
                scores[h, o] = score
                top = score if top is None else jnp.maximum(top, score)
            peak = jnp.max(top, axis=1, keepdims=True)
            accum = None
            for o in range(window + 1):
                value = v_ref[:, here] if o == 0 else vbuf[o - 1, :, here]
                both = jnp.concatenate([value, jnp.ones((rows, HEAD_DIM), bf16)], axis=1)
                weight = jnp.exp2((scores[h, o] - peak) * factor).astype(bf16)
                term = jnp.dot(weight, both, preferred_element_type=f32)
                accum = term if accum is None else accum + term
            attended[:, here] = (accum[:, :HEAD_DIM] / accum[:, HEAD_DIM:]).astype(bf16)

    def win_copy(d):
        return remote(
            win.at[:, pl.ds(0, slots)], win.at[:, pl.ds(d * slots, slots)],
            wi_s.at[d - 1], wi_r.at[d - 1], (z * ny + (y + ny - d) % ny, me),
        )

    def wout_copy(d):
        return remote(
            wout.at[pl.ds(0, slots)], wout.at[pl.ds(d * slots, slots)],
            wo_s.at[d - 1], wo_r.at[d - 1], (z * ny + (y + ny - d) % ny, me),
        )

    @pl.loop(0, groups + 1)
    def _(i):
        @pl.when(i < groups)
        def _():
            arrive(up * ny, i)
            spread(up, i, start)

        @pl.when(i == groups - 1)
        def _():
            for d in range(1, ny):
                win_copy(d).start()
            for d in range(1, ny):
                wout_copy(d).start()

        @pl.when(i > 0)
        def _():
            attend(i - 1)

    def at_z(step):
        return ((z + step) * ny + y, me)

    def at_y(d):
        return (z * ny + (y + d) % ny, me)

    def at_x(d):
        return (seq, ((chip + d) % chips) * 2 + core)

    load_proj.wait()

    size = rows // count
    half = nz // 2
    span = half * size
    parts = near_s.shape[0]
    band = rows // parts

    def block(r, target, side):
        where = pl.ds(pl.multiple_of((target * 2 + side) * width, 128), width)
        return jnp.dot(
            attended[r * band : (r + 1) * band, :], proj[:, where], preferred_element_type=f32
        )

    def far_copy(d, r):
        here = pl.ds(r * band, band)
        return remote(
            far_part.at[d - 1, here], far_near.at[d - 1, here], f_s.at[d - 1, r], f_r.at[d - 1, r],
            partner,
        )

    def cross_copy(d, c):
        here = pl.ds(c * size, size)
        return remote(
            sums.at[d - 1, here], far.at[d - 1, here], x_s.at[d - 1, c], x_r.at[d - 1, c],
            (seq, ((chip + d) % chips) * 2 + core),
        )

    def near_copy(r):
        here = pl.ds(r * band, band)
        return remote(near_part.at[here], near_near.at[here], near_s.at[r], near_r.at[r], partner)

    def square_copy(d, c):
        return remote(
            squares.at[c, me], squares.at[c, me], q_s.at[d - 1, c], q_r.at[me, c],
            (seq, (me + d) % nmp),
        )

    for r in range(parts):
        here = slice(r * band, (r + 1) * band)
        for d in range(1, chips):
            far_part[d - 1, here] = block(r, (chip + d) % chips, 1 - core).astype(bf16)
            far_copy(d, r).start()
        for d in range(1, chips):
            mine = block(r, (chip + d) % chips, core)
            far_copy(d, r).wait_recv()
            sums[d - 1, here] = (mine + far_near[d - 1, here].astype(f32)).astype(bf16)
            for c in range(r * band // size, (r + 1) * band // size):
                cross_copy(d, c).start()
    for r in range(parts):
        here = slice(r * band, (r + 1) * band)
        near_part[here, :] = block(r, chip, 1 - core).astype(bf16)
        near_copy(r).start()
        mine = block(r, chip, core)
        near_copy(r).wait_recv()
        total[here, :] = resid_ref[here, :].astype(f32) + (mine + near_near[here, :].astype(f32))

    def settle(c):
        here = slice(c * size, (c + 1) * size)
        value = total[here, :]
        for d in range(1, chips):
            cross_copy(d, c).wait_recv()
            value = value + far[d - 1, here].astype(f32)
        value = value.astype(bf16)
        state[here, :] = value
        widened = value.astype(f32)
        length = jnp.sum(widened * widened, axis=1, keepdims=True)
        flat = jnp.broadcast_to(length, (size, 128)).T[0:8, :]
        squares[c, me] = jnp.concatenate([flat] * (128 // size), axis=1)
        for d in range(1, nmp):
            square_copy(d, c).start()

    def normalize(c):
        here = slice(c * size, (c + 1) * size)
        for d in range(1, nmp):
            other = (me + d) % nmp
            remote(
                squares.at[c, other], squares.at[c, other], q_s.at[d - 1, c], q_r.at[other, c],
                partner,
            ).wait_recv()
        square = squares[c, 0]
        for k in range(1, nmp):
            square = square + squares[c, k]
        inverse = lax.rsqrt(square / (width * nmp) + epsilon)
        column = jnp.broadcast_to(inverse[0:1, 0:size], (128, size)).T[:, 0:1]
        normed[here, :] = (
            state[here, :].astype(f32) * column * gain_ref[...].astype(f32)
        ).astype(bf16)

    def own_rows(c):
        return normed.at[pl.ds(c * size, size)]

    def gather_copy(step, k, c):
        block = z - step * k
        src = own_rows(c) if k == 0 else gathered.at[c, block]
        way = 0 if step > 0 else 1
        return remote(src, gathered.at[c, block], ag_s.at[way, k, c], ag_r.at[block, c], at_z(step))

    def can_pass(step, k):
        block = z - step * k
        there = z + step
        return (block >= 0) & (block < nz) & (there >= 0) & (there < nz)

    def pass_on(k, c, steps=(1, -1)):
        for step in steps:

            @pl.when(can_pass(step, k))
            def _(step=step):
                gather_copy(step, k, c).start()

    def own_send(c):
        normalize(c)
        pass_on(0, c)

    def collect(k, c):
        if k == 1:
            gathered[c, z] = normed[pl.ds(c * size, size), :]
        for step in (1, -1):
            block = z - step * k

            @pl.when((block >= 0) & (block < nz))
            def _(step=step, block=block):
                remote(
                    gathered.at[c, block], gathered.at[c, block],
                    ag_s.at[0, 0, c], ag_r.at[block, c], partner,
                ).wait_recv()
                if k < nz - 1:
                    pass_on(k, c, (step,))

    def half_rows(side):
        return pl.ds(side * half, half)

    def pre_copy(c):
        return remote(part.at[c], near.at[c], pd_s.at[c], pd_r.at[c], partner)

    def multiply_in(c):
        other = gathered[c, half_rows(1 - core)].reshape(span, width)
        part[c] = jnp.dot(other, win[...], preferred_element_type=f32).astype(bf16)
        pre_copy(c).start()
        mine = gathered[c, half_rows(core)].reshape(span, width)
        own_part[c] = jnp.dot(mine, win[...], preferred_element_type=f32)

    def across_copy(d, c):
        return remote(
            pair.at[c, chip], pair.at[c, chip], px_s.at[d - 1, c], px_r.at[chip, c], at_x(d)
        )

    def exchange(c):
        pre_copy(c).wait_recv()
        pair[c, chip] = (own_part[c] + near[c].astype(f32)).astype(bf16)
        for d in range(1, chips):
            across_copy(d, c).start()

    def active_copy(c):
        return remote(
            active.at[c, half_rows(core)], active.at[c, half_rows(core)],
            ad_s.at[c], ad_r.at[c], partner,
        )

    def activate(c):
        for d in range(1, chips):
            other = (chip + d) % chips
            remote(
                pair.at[c, other], pair.at[c, other], px_s.at[d - 1, c], px_r.at[other, c], at_x(d)
            ).wait_recv()
        pre = pair[c, 0].astype(f32)
        for k in range(1, chips):
            pre = pre + pair[c, k].astype(f32)
        value = jnp.maximum(pre, 0.0)
        active[c, half_rows(core)] = value.astype(bf16).reshape(half, size, value.shape[1])
        active_copy(c).start()
        hot[...] += jnp.sum(value.reshape(span // 8, 8, value.shape[1]), axis=0)

    def up_copy(t, c):
        return remote(from_below.at[c, t], from_below.at[c, t], up_s.at[t, c], up_r.at[t, c], at_z(1))

    def down_copy(t, c):
        return remote(from_above.at[c, t], from_above.at[c, t], dn_s.at[t, c], dn_r.at[t, c], at_z(-1))

    def multiply_out(c):
        other = half_rows(1 - core)
        remote(active.at[c, other], active.at[c, other], ad_s.at[c], ad_r.at[c], partner).wait_recv()
        lhs = active[c].reshape(nz * size, active.shape[3])
        contrib[c] = jnp.dot(lhs, wout[...], preferred_element_type=f32).reshape(nz, size, width)

        @pl.when(z == 0)
        def _():
            for t in range(last, 0, -1):
                from_below[c, t] = contrib[c, t].astype(bf16)
                up_copy(t, c).start()

        @pl.when(z == last)
        def _():
            for t in range(last):
                from_above[c, t] = contrib[c, t].astype(bf16)
                down_copy(t, c).start()

    def middle(k, c):
        up = z + k

        @pl.when((z > 0) & (up < nz))
        def _():
            up_copy(up, c).wait_recv()
            from_below[c, up] = (contrib[c, up] + from_below[c, up].astype(f32)).astype(bf16)
            up_copy(up, c).start()

        down = z - k

        @pl.when((z < last) & (down >= 0))
        def _():
            down_copy(down, c).wait_recv()
            from_above[c, down] = (contrib[c, down] + from_above[c, down].astype(f32)).astype(bf16)
            down_copy(down, c).start()

    def finish(c):
        @pl.when(z > 0)
        def _():
            up_copy(z, c).wait_recv()
            contrib[c, z] += from_below[c, z].astype(f32)

        @pl.when(z < last)
        def _():
            down_copy(z, c).wait_recv()
            contrib[c, z] += from_above[c, z].astype(f32)

        here = pl.ds(c * size, size)
        out_ref[here, :] = (state[here, :].astype(f32) + contrib[c, z]).astype(bf16)

    hot[...] = jnp.zeros_like(hot)
    eager = min(2, count)
    for c in range(eager):
        settle(c)
        own_send(c)
    for c in range(eager, count):
        settle(c)
    for stage, k, c in ffn_order(nz, count):
        if stage == "own":
            if c >= eager:
                own_send(c)
        elif stage == "collect":
            collect(k, c)
        elif stage == "multiply_in":
            if c == 0:
                for d in range(1, ny):
                    win_copy(d).wait_recv()
            multiply_in(c)
        elif stage == "exchange":
            exchange(c)
        elif stage == "activate":
            activate(c)
        elif stage == "multiply_out":
            if c == 0:
                for d in range(1, ny):
                    wout_copy(d).wait_recv()
            multiply_out(c)
        elif stage == "middle":
            middle(k, c)

    hot_pair = remote(hot, hot_near, hp_s, hp_r, partner)
    hot_pair.start()
    hot_pair.wait_recv()
    both = jnp.sum(hot[...] + hot_near[...], axis=0, keepdims=True)
    hot_send[...] = jnp.broadcast_to(both, hot_send.shape)

    def mean_copy(d):
        return remote(
            hot_send.at[:, pl.ds(d * slots, slots)], hot_other.at[d - 1],
            hy_s.at[d - 1], hy_r.at[d - 1], at_y(d),
        )

    for d in range(1, ny):
        mean_copy(d).start()
    for c in range(count):
        finish(c)
    total = hot_send[0:1, 0:slots]
    for d in range(1, ny):
        mean_copy(d).wait_recv()
        total = total + hot_other[d - 1, 0:1, :]
    mean_ref[...] = total / total_tokens

    for c in range(count):
        for k in range(nz - 1):
            for step in (1, -1):

                @pl.when(can_pass(step, k))
                def _(step=step, k=k, c=c):
                    gather_copy(step, k, c).wait_send()

        pre_copy(c).wait_send()
        for d in range(1, chips):
            across_copy(d, c).wait_send()
        active_copy(c).wait_send()
        for t in range(nz):

            @pl.when((t > z) & (z < last))
            def _(t=t, c=c):
                up_copy(t, c).wait_send()

            @pl.when((t < z) & (z > 0))
            def _(t=t, c=c):
                down_copy(t, c).wait_send()

    for d in range(1, ny):
        win_copy(d).wait_send()
        wout_copy(d).wait_send()
        mean_copy(d).wait_send()
    hot_pair.wait_send()
    for lv in range(up + 1):
        spread(lv, None, lambda copy: copy.wait_send())

        @pl.loop(0, groups)
        def _(c, lv=lv):
            spread(lv, c, lambda copy: copy.wait_send())

    for d in range(1, chips):
        for r in range(parts):
            far_copy(d, r).wait_send()
        for c in range(count):
            cross_copy(d, c).wait_send()
    for r in range(parts):
        near_copy(r).wait_send()
    for d in range(1, nmp):
        for c in range(count):
            square_copy(d, c).wait_send()


def layer(queries, keys, values, doc_ids, resid, gain, index, live, w_in, w_out, out_proj, ny, count, collective_id):
    rows, width = queries.shape
    n = lax.axis_size("seq")
    nmp = lax.axis_size("mp")
    nz = n // ny
    chips = nmp // 2
    window = n // 2
    up = min(nz - 1, -(-window // ny))
    heads = width // HEAD_DIM
    per = 2 if heads % 2 == 0 else 1
    pieces = 1 + 2 * (heads // per)
    slots = index.shape[1]
    parts = 2
    size = rows // count
    span = (nz // 2) * size
    wide = ny * slots
    dma = pltpu.SemaphoreType.DMA
    vmem = pl.BlockSpec(memory_space=VMEM)
    anywhere = pl.BlockSpec(memory_space=pl.ANY)
    f32 = jnp.float32
    bf16 = jnp.bfloat16
    return pl.pallas_call(
        functools.partial(
            layer_kernel, nz, ny, nmp, up, window, per, count, HEAD_DIM ** (-0.5), n * rows
        ),
        out_shape=[
            jax.ShapeDtypeStruct((rows, width), bf16),
            jax.ShapeDtypeStruct((1, slots), f32),
        ],
        in_specs=[vmem] * 7 + [pl.BlockSpec(memory_space=pltpu.SMEM)] + [anywhere] * 3,
        out_specs=[vmem, vmem],
        scratch_shapes=[
            VMEM((window, rows, width), bf16),
            VMEM((window, rows, width), bf16),
            VMEM((window + 1, 1, rows), jnp.int32),
            VMEM((window + 1, rows, rows), f32),
            VMEM((per, window + 1, rows, rows), f32),
            VMEM((rows, width), bf16),
            VMEM(out_proj.shape, bf16),
            VMEM(w_out.shape, bf16),
            VMEM((width, wide), bf16),
            VMEM((wide, width), bf16),
            VMEM((chips - 1, rows, width), bf16),
            VMEM((chips - 1, rows, width), bf16),
            VMEM((chips - 1, rows, width), bf16),
            VMEM((chips - 1, rows, width), bf16),
            VMEM((rows, width), bf16),
            VMEM((rows, width), bf16),
            VMEM((rows, width), f32),
            VMEM((count, nmp, 8, 128), f32),
            VMEM((rows, width), bf16),
            VMEM((rows, width), bf16),
            VMEM((count, nz, size, width), bf16),
            VMEM((count, span, wide), bf16),
            VMEM((count, span, wide), f32),
            VMEM((count, span, wide), bf16),
            VMEM((count, chips, span, wide), bf16),
            VMEM((count, nz, size, wide), bf16),
            VMEM((count, nz, size, width), f32),
            VMEM((count, nz, size, width), bf16),
            VMEM((count, nz, size, width), bf16),
            VMEM((8, wide), f32),
            VMEM((8, wide), f32),
            VMEM((8, wide), f32),
            VMEM((ny - 1, 8, slots), f32),
            dma((3,)),
            dma((up, pieces)),
            dma((up + 1, ny - 1, pieces)),
            dma((window + 1, pieces)),
            dma((chips - 1, parts)),
            dma((chips - 1, parts)),
            dma((parts,)),
            dma((parts,)),
            dma((chips - 1, count)),
            dma((chips - 1, count)),
            dma((nmp - 1, count)),
            dma((nmp, count)),
            dma((ny - 1,)),
            dma((ny - 1,)),
            dma((ny - 1,)),
            dma((ny - 1,)),
            dma((2, nz, count)),
            dma((nz, count)),
            dma((count,)),
            dma((count,)),
            dma((chips - 1, count)),
            dma((chips, count)),
            dma((count,)),
            dma((count,)),
            dma((nz, count)),
            dma((nz, count)),
            dma((nz, count)),
            dma((nz, count)),
            dma,
            dma,
            dma((ny - 1,)),
            dma((ny - 1,)),
        ],
        compiler_params=pltpu.CompilerParams(
            collective_id=collective_id, has_side_effects=True, vmem_limit_bytes=67043328
        ),
    )(
        queries, keys, values, doc_ids[None, :], resid, gain[None, :], index, live, w_in.T, w_out, out_proj,
    )


def local(
    ny,
    resid,
    queries,
    keys,
    values,
    doc_ids,
    out_proj,
    ffn_gain,
    w_in,
    w_out,
    hot_index,
    hot_blocks,
):
    return layer(
        queries, keys, values, doc_ids, resid, ffn_gain, hot_index, hot_blocks, w_in, w_out, out_proj, ny, 4, 0
    )


def solution(mesh):
    return jax.shard_map(
        functools.partial(local, row_length(mesh)),
        mesh=mesh,
        in_specs=(
            P("seq", "mp"),
            P("seq", "mp"),
            P("seq", "mp"),
            P("seq", "mp"),
            P("seq"),
            P("mp", None),
            P("mp"),
            P("mp", "seq"),
            P("seq", "mp"),
            P("seq", None),
            P("seq"),
        ),
        out_specs=(P("seq", "mp"), P("seq", None)),
        check_vma=False,
    )
```

```python
import functools

import jax
import jax.numpy as jnp
from jax import lax
from jax.experimental import pallas as pl
from jax.experimental.pallas import tpu as pltpu
from jax.sharding import PartitionSpec as P

HEAD_DIM = 128
BLOCK = 128
MESH = pl.DeviceIdType.MESH
VMEM = pltpu.VMEM

epsilon = 1e-05
masked_score = -1e30


def row_length(mesh):
    seq = mesh.shape["seq"]
    try:
        first = [mesh.devices[i, 0].coords for i in range(seq)]
        size = len({c[1] for c in first})
        if seq % size == 0:
            return size
    except (AttributeError, IndexError, TypeError):
        pass
    return 2


def ffn_order(nz, count):
    period = 42.0 / count
    timed = []

    def put(at, stage, distance=0):
        for c in range(count):
            timed.append((at + period * c, len(timed), stage, distance, c))

    put(-16.3, "own")
    for k in range(1, nz):
        put(-5.0 + 4.5 * k, "collect", k)
    arrived = -5.0 + 4.5 * (nz - 1)
    put(arrived, "multiply_in")
    put(11.7, "exchange")
    put(18.4, "activate")
    put(22.1, "multiply_out")
    for k in range(nz - 1, 0, -1):
        put(max(38.5 - 4.5 * k, 22.1) if k < nz - 1 else 22.1, "middle", k)
    put(1000.0, "finish")
    return [entry[2:] for entry in sorted(timed)]


def layer_kernel(
    nz, ny, nmp, up, window, per, count, scale,
    q_ref, k_ref, v_ref, doc_ref, resid_ref, gain_ref, index_ref, live_ref, win_hbm, wout_hbm, proj_hbm,
    state, delta_ref, mean_ref,
    kbuf, vbuf, docs, bias, scores, attended, proj, weights, win, wout,
    far_part, far_near, sums, far, near_part, near_near, total, squares, normed,
    gathered, part, own_part, near, pair, active, contrib, from_below, from_above,
    hot, hot_near, hot_send, hot_other,
    load_sem, z_s, y_s, recv, f_s, f_r, near_s, near_r, x_s, x_r, q_s, q_r, wi_s, wi_r, wo_s, wo_r,
    ag_s, ag_r, pd_s, pd_r, px_s, px_r, ad_s, ad_r, up_s, up_r, dn_s, dn_r, hp_s, hp_r, hy_s, hy_r,
):
    f32 = jnp.float32
    bf16 = jnp.bfloat16
    seq = lax.axis_index("seq")
    me = lax.axis_index("mp")
    z = seq // ny
    y = seq % ny
    chips = nmp // 2
    chip = me // 2
    core = me % 2
    rows, width = q_ref.shape
    wide = per * HEAD_DIM
    groups = width // wide
    slots = index_ref.shape[1]
    last = nz - 1
    partner = (seq, chip * 2 + 1 - core)

    barrier = pltpu.get_barrier_semaphore()

    def greet(where):
        pl.semaphore_signal(barrier, inc=1, device_id=where, device_id_type=MESH)

    above = ((z + 1) * ny + y, me)

    @pl.when(z > 0)
    def _():
        greet(((z - 1) * ny + y, me))

    @pl.when(z < last)
    def _():
        greet(above)

    for d in range(1, nmp):
        greet((seq, (me + d) % nmp))
    for d in range(1, ny):
        greet((z * ny + (y + d) % ny, me))
    has_below = jnp.where(z > 0, 1, 0)
    has_above = jnp.where(z < last, 1, 0)
    pl.semaphore_wait(barrier, has_below + has_above + nmp + ny - 2)

    def remote(src, dst, send, got, where):
        return pltpu.make_async_remote_copy(
            src_ref=src, dst_ref=dst, send_sem=send, recv_sem=got,
            device_id=where, device_id_type=MESH,
        )

    def cols(c):
        return pl.ds(pl.multiple_of(c * wide, 128), wide)

    def pieces(lv, c):
        slot = lv * ny - 1
        if lv == 0:
            return k_ref.at[:, cols(c)], v_ref.at[:, cols(c)]
        return kbuf.at[slot, :, cols(c)], vbuf.at[slot, :, cols(c)]

    def landing(o, c):
        return kbuf.at[o - 1, :, cols(c)], vbuf.at[o - 1, :, cols(c)]

    def copies(lv, o, c, send, where):
        if c is None:
            src = doc_ref if lv == 0 else docs.at[lv * ny]
            return [remote(src, docs.at[o], send.at[0], recv.at[o, 0], where)]
        out = []
        for j, (src, dst) in enumerate(zip(pieces(lv, c), landing(o, c))):
            p = 1 + 2 * c + j
            out.append(remote(src, dst, send.at[p], recv.at[o, p], where))
        return out

    def z_copies(lv, c):
        return copies(lv, (lv + 1) * ny, c, z_s.at[lv], above)

    def y_copies(lv, d, c):
        other = (y + d) % ny
        return copies(lv, lv * ny + other - y, c, y_s.at[lv, d - 1], (z * ny + other, me))

    def holds(lv):
        return z >= lv

    def y_wanted(lv, d):
        o = lv * ny + (y + d) % ny - y
        return holds(lv) & (o >= 0) & (o <= window)

    def spread(lv, c, act):
        if lv < up:

            @pl.when(holds(lv) & (z < last))
            def _():
                for copy in z_copies(lv, c):
                    act(copy)

        for d in range(1, ny):

            @pl.when(y_wanted(lv, d))
            def _(d=d):
                for copy in y_copies(lv, d, c):
                    act(copy)

    def start(copy):
        copy.start()

    def arrive(o, c):
        @pl.when(seq >= o)
        def _():
            if c is None:
                remote(docs.at[o], docs.at[o], z_s.at[0, 0], recv.at[o, 0], partner).wait_recv()
                return
            for j, dst in enumerate(landing(o, c)):
                p = 1 + 2 * c + j
                remote(dst, dst, z_s.at[0, p], recv.at[o, p], partner).wait_recv()

    spread(0, None, start)
    spread(0, 0, start)
    load_in = pltpu.make_async_copy(win_hbm, weights, load_sem.at[0])
    load_in.start()
    load_proj = pltpu.make_async_copy(proj_hbm, proj, load_sem.at[2])
    load_proj.start()
    for o in range(1, window + 1):

        @pl.when(seq < o)
        def _(o=o):
            kbuf[o - 1] = jnp.zeros((rows, width), bf16)
            vbuf[o - 1] = jnp.zeros((rows, width), bf16)
            docs[o] = jnp.full(docs.shape[1:], -1, jnp.int32)

    docs[0] = doc_ref[...]
    arrive(ny, None)
    spread(1, None, start)
    for c in range(1, groups):
        spread(0, c, start)

    load_in.wait()
    hidden = weights.shape[0]
    order = lax.broadcasted_iota(jnp.int32, (1, slots), 1)
    chosen = jnp.where(order < BLOCK * live_ref[0], index_ref[...], -1).astype(f32)
    chosen = jnp.broadcast_to(chosen, (BLOCK, slots))
    neurons = lax.broadcasted_iota(jnp.int32, (BLOCK, hidden), 1).astype(f32)

    def picked(r):
        here = slice(r * BLOCK, (r + 1) * BLOCK)
        picks = (neurons == chosen[:, here].T[:, 0:1]).astype(f32).astype(bf16)
        return jnp.dot(picks, weights[...], preferred_element_type=f32)

    for r in range(slots // BLOCK):
        win[:, r * BLOCK : (r + 1) * BLOCK] = picked(r).T.astype(bf16)
    load_out = pltpu.make_async_copy(wout_hbm, weights, load_sem.at[1])
    load_out.start()
    load_out.wait()
    for r in range(slots // BLOCK):
        wout[r * BLOCK : (r + 1) * BLOCK, :] = picked(r).astype(bf16)

    for lv in range(1, up):

        @pl.loop(0, groups)
        def _(c, lv=lv):
            arrive(lv * ny, c)
            spread(lv, c, start)

    for lv in range(2, up + 1):
        arrive(lv * ny, None)
        spread(lv, None, start)
    for o in range(1, window + 1):
        if o % ny:
            arrive(o, None)
    row = lax.broadcasted_iota(jnp.int32, (rows, rows), 0)
    col = lax.broadcasted_iota(jnp.int32, (rows, rows), 1)
    mine = jnp.broadcast_to(doc_ref[...].astype(f32), (128, rows)).T[:, 0:1]
    for o in range(window + 1):
        seen = mine == docs[o].astype(f32)
        if o == 0:
            seen = seen & (row >= col)
        bias[o] = jnp.where(seen, 0.0, masked_score)

    factor = scale * 1.4426950408889634

    def attend(c):
        for o in range(1, window + 1):
            if o % ny:
                arrive(o, c)
        for h in range(per):
            here = pl.ds(pl.multiple_of(c * wide + h * HEAD_DIM, HEAD_DIM), HEAD_DIM)
            query = q_ref[:, here]
            top = None
            for o in range(window + 1):
                key = k_ref[:, here] if o == 0 else kbuf[o - 1, :, here]
                score = lax.dot_general(
                    query, key, (((1,), (1,)), ((), ())), preferred_element_type=f32
                ) + bias[o]
                scores[h, o] = score
                top = score if top is None else jnp.maximum(top, score)
            peak = jnp.max(top, axis=1, keepdims=True)
            accum = None
            for o in range(window + 1):
                value = v_ref[:, here] if o == 0 else vbuf[o - 1, :, here]
                both = jnp.concatenate([value, jnp.ones((rows, HEAD_DIM), bf16)], axis=1)
                weight = jnp.exp2((scores[h, o] - peak) * factor).astype(bf16)
                term = jnp.dot(weight, both, preferred_element_type=f32)
                accum = term if accum is None else accum + term
            attended[:, here] = (accum[:, :HEAD_DIM] / accum[:, HEAD_DIM:]).astype(bf16)

    def win_copy(d):
        return remote(
            win.at[:, pl.ds(0, slots)], win.at[:, pl.ds(d * slots, slots)],
            wi_s.at[d - 1], wi_r.at[d - 1], (z * ny + (y + ny - d) % ny, me),
        )

    def wout_copy(d):
        return remote(
            wout.at[pl.ds(0, slots)], wout.at[pl.ds(d * slots, slots)],
            wo_s.at[d - 1], wo_r.at[d - 1], (z * ny + (y + ny - d) % ny, me),
        )

    @pl.loop(0, groups + 1)
    def _(i):
        @pl.when(i < groups)
        def _():
            arrive(up * ny, i)
            spread(up, i, start)

        @pl.when(i == groups - 1)
        def _():
            for d in range(1, ny):
                win_copy(d).start()
            for d in range(1, ny):
                wout_copy(d).start()

        @pl.when(i > 0)
        def _():
            attend(i - 1)

    def at_z(step):
        return ((z + step) * ny + y, me)

    def at_y(d):
        return (z * ny + (y + d) % ny, me)

    def at_x(d):
        return (seq, ((chip + d) % chips) * 2 + core)

    load_proj.wait()

    size = rows // count
    half = nz // 2
    span = half * size
    parts = near_s.shape[0]
    band = rows // parts

    def block(r, target, side):
        where = pl.ds(pl.multiple_of((target * 2 + side) * width, 128), width)
        return jnp.dot(
            attended[r * band : (r + 1) * band, :], proj[:, where], preferred_element_type=f32
        )

    def far_copy(d, r):
        here = pl.ds(r * band, band)
        return remote(
            far_part.at[d - 1, here], far_near.at[d - 1, here], f_s.at[d - 1, r], f_r.at[d - 1, r],
            partner,
        )

    def cross_copy(d, c):
        here = pl.ds(c * size, size)
        return remote(
            sums.at[d - 1, here], far.at[d - 1, here], x_s.at[d - 1, c], x_r.at[d - 1, c],
            (seq, ((chip + d) % chips) * 2 + core),
        )

    def near_copy(r):
        here = pl.ds(r * band, band)
        return remote(near_part.at[here], near_near.at[here], near_s.at[r], near_r.at[r], partner)

    def square_copy(d, c):
        return remote(
            squares.at[c, me], squares.at[c, me], q_s.at[d - 1, c], q_r.at[me, c],
            (seq, (me + d) % nmp),
        )

    for r in range(parts):
        here = slice(r * band, (r + 1) * band)
        for d in range(1, chips):
            far_part[d - 1, here] = block(r, (chip + d) % chips, 1 - core).astype(bf16)
            far_copy(d, r).start()
        for d in range(1, chips):
            mine = block(r, (chip + d) % chips, core)
            far_copy(d, r).wait_recv()
            sums[d - 1, here] = (mine + far_near[d - 1, here].astype(f32)).astype(bf16)
            for c in range(r * band // size, (r + 1) * band // size):
                cross_copy(d, c).start()
    for r in range(parts):
        here = slice(r * band, (r + 1) * band)
        near_part[here, :] = block(r, chip, 1 - core).astype(bf16)
        near_copy(r).start()
        mine = block(r, chip, core)
        near_copy(r).wait_recv()
        total[here, :] = resid_ref[here, :].astype(f32) + (mine + near_near[here, :].astype(f32))

    def settle(c):
        here = slice(c * size, (c + 1) * size)
        value = total[here, :]
        for d in range(1, chips):
            cross_copy(d, c).wait_recv()
            value = value + far[d - 1, here].astype(f32)
        value = value.astype(bf16)
        state[here, :] = value
        widened = value.astype(f32)
        length = jnp.sum(widened * widened, axis=1, keepdims=True)
        flat = jnp.broadcast_to(length, (size, 128)).T[0:8, :]
        squares[c, me] = jnp.concatenate([flat] * (128 // size), axis=1)
        for d in range(1, nmp):
            square_copy(d, c).start()

    gains = gain_ref[...].astype(f32).reshape(1, width)

    def normalize(c):
        here = slice(c * size, (c + 1) * size)
        for d in range(1, nmp):
            other = (me + d) % nmp
            remote(
                squares.at[c, other], squares.at[c, other], q_s.at[d - 1, c], q_r.at[other, c],
                partner,
            ).wait_recv()
        square = squares[c, 0]
        for k in range(1, nmp):
            square = square + squares[c, k]
        inverse = lax.rsqrt(square / (width * nmp) + epsilon)
        column = jnp.broadcast_to(inverse[0:1, 0:size], (128, size)).T[:, 0:1]
        normed[here, :] = (
            state[here, :].astype(f32) * column * gains
        ).astype(bf16)

    def own_rows(c):
        return normed.at[pl.ds(c * size, size)]

    def gather_copy(step, k, c):
        block = z - step * k
        src = own_rows(c) if k == 0 else gathered.at[c, block]
        way = 0 if step > 0 else 1
        return remote(src, gathered.at[c, block], ag_s.at[way, k, c], ag_r.at[block, c], at_z(step))

    def can_pass(step, k):
        block = z - step * k
        there = z + step
        return (block >= 0) & (block < nz) & (there >= 0) & (there < nz)

    def pass_on(k, c, steps=(1, -1)):
        for step in steps:

            @pl.when(can_pass(step, k))
            def _(step=step):
                gather_copy(step, k, c).start()

    def own_send(c):
        normalize(c)
        pass_on(0, c)

    def collect(k, c):
        if k == 1:
            gathered[c, z] = normed[pl.ds(c * size, size), :]
        for step in (1, -1):
            block = z - step * k

            @pl.when((block >= 0) & (block < nz))
            def _(step=step, block=block):
                remote(
                    gathered.at[c, block], gathered.at[c, block],
                    ag_s.at[0, 0, c], ag_r.at[block, c], partner,
                ).wait_recv()
                if k < nz - 1:
                    pass_on(k, c, (step,))

    def half_rows(side):
        return pl.ds(side * half, half)

    def pre_copy(c):
        return remote(part.at[c], near.at[c], pd_s.at[c], pd_r.at[c], partner)

    def multiply_in(c):
        other = gathered[c, half_rows(1 - core)].reshape(span, width)
        part[c] = jnp.dot(other, win[...], preferred_element_type=f32).astype(bf16)
        pre_copy(c).start()
        mine = gathered[c, half_rows(core)].reshape(span, width)
        own_part[c] = jnp.dot(mine, win[...], preferred_element_type=f32)

    def across_copy(d, c):
        return remote(
            pair.at[c, chip], pair.at[c, chip], px_s.at[d - 1, c], px_r.at[chip, c], at_x(d)
        )

    def exchange(c):
        pre_copy(c).wait_recv()
        pair[c, chip] = (own_part[c] + near[c].astype(f32)).astype(bf16)
        for d in range(1, chips):
            across_copy(d, c).start()

    def active_copy(c):
        return remote(
            active.at[c, half_rows(core)], active.at[c, half_rows(core)],
            ad_s.at[c], ad_r.at[c], partner,
        )

    def activate(c):
        for d in range(1, chips):
            other = (chip + d) % chips
            remote(
                pair.at[c, other], pair.at[c, other], px_s.at[d - 1, c], px_r.at[other, c], at_x(d)
            ).wait_recv()
        pre = pair[c, 0].astype(f32)
        for k in range(1, chips):
            pre = pre + pair[c, k].astype(f32)
        value = jnp.maximum(pre, 0.0)
        active[c, half_rows(core)] = value.astype(bf16).reshape(half, size, value.shape[1])
        active_copy(c).start()
        hot[...] += jnp.sum(value.reshape(span // 8, 8, value.shape[1]), axis=0)

    def up_copy(t, c):
        return remote(from_below.at[c, t], from_below.at[c, t], up_s.at[t, c], up_r.at[t, c], at_z(1))

    def down_copy(t, c):
        return remote(from_above.at[c, t], from_above.at[c, t], dn_s.at[t, c], dn_r.at[t, c], at_z(-1))

    def multiply_out(c):
        other = half_rows(1 - core)
        remote(active.at[c, other], active.at[c, other], ad_s.at[c], ad_r.at[c], partner).wait_recv()
        lhs = active[c].reshape(nz * size, active.shape[3])
        contrib[c] = jnp.dot(lhs, wout[...], preferred_element_type=f32).reshape(nz, size, width)

        @pl.when(z == 0)
        def _():
            for t in range(last, 0, -1):
                from_below[c, t] = contrib[c, t].astype(bf16)
                up_copy(t, c).start()

        @pl.when(z == last)
        def _():
            for t in range(last):
                from_above[c, t] = contrib[c, t].astype(bf16)
                down_copy(t, c).start()

    def middle(k, c):
        up = z + k

        @pl.when((z > 0) & (up < nz))
        def _():
            up_copy(up, c).wait_recv()
            from_below[c, up] = (contrib[c, up] + from_below[c, up].astype(f32)).astype(bf16)
            up_copy(up, c).start()

        down = z - k

        @pl.when((z < last) & (down >= 0))
        def _():
            down_copy(down, c).wait_recv()
            from_above[c, down] = (contrib[c, down] + from_above[c, down].astype(f32)).astype(bf16)
            down_copy(down, c).start()

    def finish(c):
        @pl.when(z > 0)
        def _():
            up_copy(z, c).wait_recv()
            contrib[c, z] += from_below[c, z].astype(f32)

        @pl.when(z < last)
        def _():
            down_copy(z, c).wait_recv()
            contrib[c, z] += from_above[c, z].astype(f32)

        here = pl.ds(c * size, size)
        delta_ref[here, :] = contrib[c, z]

    hot[...] = jnp.zeros_like(hot)
    eager = min(2, count)
    for c in range(eager):
        settle(c)
        own_send(c)
    for c in range(eager, count):
        settle(c)
    for stage, k, c in ffn_order(nz, count):
        if stage == "own":
            if c >= eager:
                own_send(c)
        elif stage == "collect":
            collect(k, c)
        elif stage == "multiply_in":
            if c == 0:
                for d in range(1, ny):
                    win_copy(d).wait_recv()
            multiply_in(c)
        elif stage == "exchange":
            exchange(c)
        elif stage == "activate":
            activate(c)
        elif stage == "multiply_out":
            if c == 0:
                for d in range(1, ny):
                    wout_copy(d).wait_recv()
            multiply_out(c)
        elif stage == "middle":
            middle(k, c)

    hot_pair = remote(hot, hot_near, hp_s, hp_r, partner)
    hot_pair.start()
    hot_pair.wait_recv()
    both = jnp.sum(hot[...] + hot_near[...], axis=0, keepdims=True)
    hot_send[...] = jnp.broadcast_to(both, hot_send.shape)

    def mean_copy(d):
        return remote(
            hot_send.at[:, pl.ds(d * slots, slots)], hot_other.at[d - 1],
            hy_s.at[d - 1], hy_r.at[d - 1], at_y(d),
        )

    for d in range(1, ny):
        mean_copy(d).start()
    for c in range(count):
        finish(c)
    total = hot_send[0:1, 0:slots]
    for d in range(1, ny):
        mean_copy(d).wait_recv()
        total = total + hot_other[d - 1, 0:1, :]
    mean_ref[...] = total

    for c in range(count):
        for k in range(nz - 1):
            for step in (1, -1):

                @pl.when(can_pass(step, k))
                def _(step=step, k=k, c=c):
                    gather_copy(step, k, c).wait_send()

        pre_copy(c).wait_send()
        for d in range(1, chips):
            across_copy(d, c).wait_send()
        active_copy(c).wait_send()
        for t in range(nz):

            @pl.when((t > z) & (z < last))
            def _(t=t, c=c):
                up_copy(t, c).wait_send()

            @pl.when((t < z) & (z > 0))
            def _(t=t, c=c):
                down_copy(t, c).wait_send()

    for d in range(1, ny):
        win_copy(d).wait_send()
        wout_copy(d).wait_send()
        mean_copy(d).wait_send()
    hot_pair.wait_send()
    for lv in range(up + 1):
        spread(lv, None, lambda copy: copy.wait_send())

        @pl.loop(0, groups)
        def _(c, lv=lv):
            spread(lv, c, lambda copy: copy.wait_send())

    for d in range(1, chips):
        for r in range(parts):
            far_copy(d, r).wait_send()
        for c in range(count):
            cross_copy(d, c).wait_send()
    for r in range(parts):
        near_copy(r).wait_send()
    for d in range(1, nmp):
        for c in range(count):
            square_copy(d, c).wait_send()


def layer(queries, keys, values, doc_ids, resid, gain, index, live, w_in, w_out, out_proj, ny, count, collective_id):
    rows, width = queries.shape
    n = lax.axis_size("seq")
    nmp = lax.axis_size("mp")
    nz = n // ny
    chips = nmp // 2
    window = n // 2
    up = min(nz - 1, -(-window // ny))
    heads = width // HEAD_DIM
    per = 2 if heads % 2 == 0 else 1
    pieces = 1 + 2 * (heads // per)
    slots = index.shape[1]
    parts = 2
    size = rows // count
    span = (nz // 2) * size
    wide = ny * slots
    dma = pltpu.SemaphoreType.DMA
    vmem = pl.BlockSpec(memory_space=VMEM)
    anywhere = pl.BlockSpec(memory_space=pl.ANY)
    f32 = jnp.float32
    bf16 = jnp.bfloat16
    return pl.pallas_call(
        functools.partial(
            layer_kernel, nz, ny, nmp, up, window, per, count, HEAD_DIM ** (-0.5)
        ),
        out_shape=[
            jax.ShapeDtypeStruct((rows, width), bf16),
            jax.ShapeDtypeStruct((rows, width), f32),
            jax.ShapeDtypeStruct((1, slots), f32),
        ],
        in_specs=[vmem] * 7 + [pl.BlockSpec(memory_space=pltpu.SMEM)] + [anywhere] * 3,
        out_specs=[vmem, vmem, vmem],
        scratch_shapes=[
            VMEM((window, rows, width), bf16),
            VMEM((window, rows, width), bf16),
            VMEM((window + 1, 1, rows), jnp.int32),
            VMEM((window + 1, rows, rows), f32),
            VMEM((per, window + 1, rows, rows), f32),
            VMEM((rows, width), bf16),
            VMEM(out_proj.shape, bf16),
            VMEM(w_out.shape, bf16),
            VMEM((width, wide), bf16),
            VMEM((wide, width), bf16),
            VMEM((chips - 1, rows, width), bf16),
            VMEM((chips - 1, rows, width), bf16),
            VMEM((chips - 1, rows, width), bf16),
            VMEM((chips - 1, rows, width), bf16),
            VMEM((rows, width), bf16),
            VMEM((rows, width), bf16),
            VMEM((rows, width), f32),
            VMEM((count, nmp, 8, 128), f32),
            VMEM((rows, width), bf16),
            VMEM((count, nz, size, width), bf16),
            VMEM((count, span, wide), bf16),
            VMEM((count, span, wide), f32),
            VMEM((count, span, wide), bf16),
            VMEM((count, chips, span, wide), bf16),
            VMEM((count, nz, size, wide), bf16),
            VMEM((count, nz, size, width), f32),
            VMEM((count, nz, size, width), bf16),
            VMEM((count, nz, size, width), bf16),
            VMEM((8, wide), f32),
            VMEM((8, wide), f32),
            VMEM((8, wide), f32),
            VMEM((ny - 1, 8, slots), f32),
            dma((3,)),
            dma((up, pieces)),
            dma((up + 1, ny - 1, pieces)),
            dma((window + 1, pieces)),
            dma((chips - 1, parts)),
            dma((chips - 1, parts)),
            dma((parts,)),
            dma((parts,)),
            dma((chips - 1, count)),
            dma((chips - 1, count)),
            dma((nmp - 1, count)),
            dma((nmp, count)),
            dma((ny - 1,)),
            dma((ny - 1,)),
            dma((ny - 1,)),
            dma((ny - 1,)),
            dma((2, nz, count)),
            dma((nz, count)),
            dma((count,)),
            dma((count,)),
            dma((chips - 1, count)),
            dma((chips, count)),
            dma((count,)),
            dma((count,)),
            dma((nz, count)),
            dma((nz, count)),
            dma((nz, count)),
            dma((nz, count)),
            dma,
            dma,
            dma((ny - 1,)),
            dma((ny - 1,)),
        ],
        compiler_params=pltpu.CompilerParams(
            collective_id=collective_id, has_side_effects=True, vmem_limit_bytes=67043328
        ),
    )(
        queries, keys, values, doc_ids[None, :], resid, gain, index, live, w_in.T, w_out, out_proj,
    )


def local(
    ny,
    resid,
    queries,
    keys,
    values,
    doc_ids,
    out_proj,
    ffn_gain,
    w_in,
    w_out,
    hot_index,
    hot_blocks,
):
    state, delta, sums = layer(
        queries, keys, values, doc_ids, resid, ffn_gain, hot_index, hot_blocks, w_in, w_out, out_proj, ny, 4, 0
    )
    total_tokens = resid.shape[0] * lax.axis_size("seq")
    return (state.astype(jnp.float32) + delta).astype(jnp.bfloat16), sums / total_tokens


def solution(mesh):
    return jax.shard_map(
        functools.partial(local, row_length(mesh)),
        mesh=mesh,
        in_specs=(
            P("seq", "mp"),
            P("seq", "mp"),
            P("seq", "mp"),
            P("seq", "mp"),
            P("seq"),
            P("mp", None),
            P("mp"),
            P("mp", "seq"),
            P("seq", "mp"),
            P("seq", None),
            P("seq"),
        ),
        out_specs=(P("seq", "mp"), P("seq", None)),
        check_vma=False,
    )
```
